16 devices in a mesh: rep: 1, dp: 16 (over x, y, z, core).
Axes of the slice: x: 2, y: 2, z: 2, core: 2. Of those that a mesh axis runs over, the one named last changes fastest.
Arguments:
- x: bfloat16 [16, 2048, 1024], P(('rep', 'dp'))
- dy: bfloat16 [16, 2048, 1024], P(('rep', 'dp'))
- w_gate: bfloat16 [2, 1024, 2816], replicated
- w_up: bfloat16 [2, 1024, 2816], replicated
- w_down: bfloat16 [2, 2816, 1024], replicated
- m_w_gate: float32 [2, 1024, 2816], P(None, 'dp')
- m_w_up: float32 [2, 1024, 2816], P(None, 'dp')
- m_w_down: float32 [2, 2816, 1024], P(None, 'dp')
- v_w_gate: float32 [2, 1024, 2816], P(None, 'dp')
- v_w_up: float32 [2, 1024, 2816], P(None, 'dp')
- v_w_down: float32 [2, 2816, 1024], P(None, 'dp')
Outputs:
- output 1: bfloat16 [2, 1024, 2816], P('rep')
- output 2: bfloat16 [2, 1024, 2816], P('rep')
- output 3: bfloat16 [2, 2816, 1024], P('rep')
- output 4: float32 [2, 1024, 2816], P('rep', 'dp')
- output 5: float32 [2, 1024, 2816], P('rep', 'dp')
- output 6: float32 [2, 2816, 1024], P('rep', 'dp')
- output 7: float32 [2, 1024, 2816], P('rep', 'dp')
- output 8: float32 [2, 1024, 2816], P('rep', 'dp')
- output 9: float32 [2, 2816, 1024], P('rep', 'dp')
All inputs are finite; a program needn't handle non-finite values.
Results may differ from the reference program's by a relative error of at most 0.022.
Values are sent between devices in bfloat16 or wider.
A program may use at most 2 GiB of HBM per device.

```python
import jax
import jax.numpy as jnp
from jax import lax

SEQUENCES = 16
TOKENS = 2048
D = 1024
FF = 2816
LAYERS = 2
NAMES = ("w_gate", "w_up", "w_down")
SHAPES = {"w_gate": (LAYERS, D, FF), "w_up": (LAYERS, D, FF), "w_down": (LAYERS, FF, D)}


def bump(key, n, height):
    away = (jnp.arange(n, dtype=jnp.int32) - jax.random.randint(key, (), 0, n, jnp.int32)) % n
    return jnp.where(away < n // 8, height, 1.0)


def together(key, own, strength):
    shared = jax.random.normal(key, own.shape[1:], jnp.float32)
    return (own + strength * shared) * lax.rsqrt(1 + strength * strength)


def setup_inputs(seed: int = 0, part: int = 0) -> dict:
    kx, kdy, ka, kb, kz, kf, kh, kl, *keys = jax.random.split(jax.random.key(seed), 8 + 3 * len(NAMES))
    kx, kdy, ka, kb = (jax.random.fold_in(k, part) for k in (kx, kdy, ka, kb))
    kw, km, kv = (keys[i::3] for i in range(3))
    shape = (SEQUENCES, TOKENS, D)
    much_x, much_dy = jax.random.uniform(kz, (2,), jnp.float32, 0.0, 1.0)
    loud = 2.0 ** jax.random.uniform(jax.random.fold_in(kz, 1), (), jnp.float32, -1.0, 2.0)
    layers = 2.0 ** jax.random.uniform(kl, (LAYERS, 1, 1), jnp.float32, -1.0, 1.0)
    x = together(ka, jax.random.normal(kx, shape, jnp.float32), much_x) * bump(kf, D, 4.0)
    dy = together(kb, jax.random.normal(kdy, shape, jnp.float32), much_dy)
    drawn = {"x": x.astype(jnp.bfloat16), "dy": (loud * dy * (SEQUENCES * TOKENS) ** -0.5).astype(jnp.bfloat16)}
    for key, name in zip(kw, NAMES, strict=True):
        w = jax.random.normal(key, SHAPES[name], jnp.float32) * SHAPES[name][1] ** -0.5
        drawn[name] = (w * {"w_gate": 1.0, "w_up": bump(kh, FF, 4.0), "w_down": layers}[name]).astype(jnp.bfloat16)
    for key, name in zip(km, NAMES, strict=True):
        drawn[f"m_{name}"] = 0.1 * jax.random.normal(key, SHAPES[name], jnp.float32)
    for key, name in zip(kv, NAMES, strict=True):
        drawn[f"v_{name}"] = jax.random.uniform(key, SHAPES[name], jnp.float32, 0.005, 0.015)
    return drawn


def matmul(a, w):
    return jnp.dot(a, w, preferred_element_type=jnp.float32).astype(jnp.bfloat16)


def normed(h):
    wide = h.astype(jnp.float32)
    scale = lax.rsqrt(jnp.mean(wide**2, -1, keepdims=True) + 1e-6)
    return (wide * scale).astype(jnp.bfloat16)


def layer(h, w):
    a = normed(h)
    gate = jnp.dot(a, w["w_gate"], preferred_element_type=jnp.float32)
    up = jnp.dot(a, w["w_up"], preferred_element_type=jnp.float32)
    return h + matmul((jax.nn.silu(gate) * up).astype(jnp.bfloat16), w["w_down"])


def adamw(w, m, v, g):
    m = 0.9 * m + 0.1 * g
    v = 0.95 * v + 0.05 * g * g
    step = m * lax.rsqrt(v + 1e-8) + 0.1 * w
    return (w - 0.02 * step).astype(jnp.bfloat16), m, v


def clipped(gradients, sum_of_squares, count):
    factor = jnp.minimum(1.0, 0.5 * lax.rsqrt(sum_of_squares / count + 1e-30))
    return [g * factor for g in gradients]


def stack(weights, h):
    return lax.scan(lambda h, w: (layer(h, w), None), h, weights)[0]


def reference(x, dy, w_gate, w_up, w_down, m_w_gate, m_w_up, m_w_down, v_w_gate, v_w_up, v_w_down):
    weights = dict(zip(NAMES, (w_gate, w_up, w_down), strict=True))

    def take(so_far, sequence):
        h, by_y = sequence
        _, back = jax.vjp(lambda w: stack(w, h), weights)
        return jax.tree.map(lambda total, term: total + term.astype(jnp.float32), so_far, back(by_y)[0]), None

    none_yet = {name: jnp.zeros(w.shape, jnp.float32) for name, w in weights.items()}
    by_weights, _ = lax.scan(take, none_yet, (x, dy))
    gradients = [by_weights[name].astype(jnp.bfloat16).astype(jnp.float32) for name in NAMES]
    gradients = clipped(gradients, sum(jnp.sum(g * g) for g in gradients), sum(g.size for g in gradients))
    new = [
        adamw(w.astype(jnp.float32), m, v, g)
        for w, m, v, g in zip((w_gate, w_up, w_down), (m_w_gate, m_w_up, m_w_down), (v_w_gate, v_w_up, v_w_down), gradients, strict=True)
    ]
    return tuple(one[which] for which in range(3) for one in new)
```

```python
import jax
import jax.numpy as jnp
from jax import lax
from jax.sharding import PartitionSpec as P

NAMES = ("w_gate", "w_up", "w_down")


def dot(a, b, dims):
    return lax.dot_general(a, b, (dims, ((), ())), preferred_element_type=jnp.float32)


def adamw(w, m, v, g):
    m = 0.9 * m + 0.1 * g
    v = 0.95 * v + 0.05 * g * g
    step = m * lax.rsqrt(v + 1e-8) + 0.1 * w
    return (w - 0.02 * step).astype(jnp.bfloat16), m, v


def solution(mesh):
    n = mesh.shape["dp"]

    def step(x, dy, w_gate, w_up, w_down, *moments):
        m, v = moments[:3], moments[3:]
        layers = w_gate.shape[0]
        h = x[0]
        saved = []
        for l in range(layers):
            wide = h.astype(jnp.float32)
            scale = lax.rsqrt(jnp.mean(wide**2, -1, keepdims=True) + 1e-6)
            a = (wide * scale).astype(jnp.bfloat16)
            gate = dot(a, w_gate[l], ((1,), (0,)))
            up = dot(a, w_up[l], ((1,), (0,)))
            z = (jax.nn.silu(gate) * up).astype(jnp.bfloat16)
            saved.append((h, scale, a, gate, up, z))
            if l + 1 < layers:
                h = h + dot(z, w_down[l], ((1,), (0,))).astype(jnp.bfloat16)
        d = dy[0]
        shards = {name: [None] * layers for name in NAMES}

        def scatter(t):
            return lax.psum_scatter(t.astype(jnp.bfloat16), "dp", scatter_dimension=0, tiled=True)

        for l in reversed(range(layers)):
            h, scale, a, gate, up, z = saved[l]
            shards["w_down"][l] = scatter(dot(z, d, ((0,), (0,))))
            dz = dot(d, w_down[l], ((1,), (1,))).astype(jnp.bfloat16).astype(jnp.float32)
            sig = jax.nn.sigmoid(gate)
            silu = gate * sig
            dup = (dz * silu).astype(jnp.bfloat16)
            dgate = (dz * up * (sig * (1 + gate * (1 - sig)))).astype(jnp.bfloat16)
            shards["w_gate"][l] = scatter(dot(a, dgate, ((0,), (0,))))
            shards["w_up"][l] = scatter(dot(a, dup, ((0,), (0,))))
            if l:
                da = dot(dgate, w_gate[l], ((1,), (1,))) + dot(dup, w_up[l], ((1,), (1,)))
                wide = h.astype(jnp.float32)
                back = da * scale - wide * (scale**3 * jnp.mean(da * wide, -1, keepdims=True))
                d = d + back.astype(jnp.bfloat16)

        g = [[t.astype(jnp.float32) for t in shards[name]] for name in NAMES]
        total = lax.psum(sum(jnp.sum(t * t) for ts in g for t in ts), "dp")
        count = sum(t.size for ts in g for t in ts) * n
        factor = jnp.minimum(1.0, 0.5 * lax.rsqrt(total / count + 1e-30))
        me = lax.axis_index("dp")
        new = []
        for w, mm, vv, ts in zip((w_gate, w_up, w_down), m, v, g, strict=True):
            rows = mm.shape[1]
            own = lax.dynamic_slice_in_dim(w, me * rows, rows, 1).astype(jnp.float32)
            nw, nm, nv = adamw(own, mm, vv, jnp.stack(ts) * factor)
            new.append((lax.all_gather(nw, "dp", axis=1, tiled=True), nm, nv))
        return tuple(one[which] for which in range(3) for one in new)

    seq, whole, rows = P(("rep", "dp"), None, None), P(), P(None, "dp", None)
    return jax.shard_map(
        step,
        mesh=mesh,
        in_specs=(seq, seq) + (whole,) * 3 + (rows,) * 6,
        out_specs=(P("rep", None, None),) * 3 + (P("rep", "dp", None),) * 6,
        check_vma=False,
    )
```

```python
import functools

import jax
import jax.numpy as jnp
from jax import lax
from jax.experimental import pallas as pl
from jax.experimental.pallas import tpu as pltpu
from jax.sharding import PartitionSpec as P

MESH = pl.DeviceIdType.MESH

NAMES = ("w_gate", "w_up", "w_down")


def dot(a, b, dims):
    return lax.dot_general(a, b, (dims, ((), ())), preferred_element_type=jnp.float32)


LINKS = (8, 4, 2)


def flipped(me, stride):
    return me + stride - 2 * stride * ((me // stride) % 2)


def widths(columns, turn):
    lanes = columns // 128
    sizes = [128 * ((lanes + (k + turn) % 3) // 3) for k in range(3)]
    starts = [0, sizes[0], sizes[0] + sizes[1]]
    return list(zip(starts, sizes))


def gather_kernel(shapes, count, sq, *refs):
    n_mat = len(shapes)
    g, w, m, v, new_w, new_m, new_v, own_w, out_w, out_m, out_v = (refs[i * n_mat : (i + 1) * n_mat] for i in range(11))
    squares, sq_send, sq_recv, in_sem, keep_sem, mv_sem, ici_send, ici_recv, d2d_send, d2d_recv = refs[11 * n_mat :]
    me = lax.axis_index("dp")
    at = [(me // s) % 2 for s in LINKS]
    core = me % 2
    units = [(i, l) for l in reversed(range(shapes[0][0])) for i in range(n_mat)]

    loads = [pltpu.make_async_copy(w[i].at[l, me], own_w[i].at[l], in_sem.at[u]) for u, (i, l) in enumerate(units)]
    for copy in loads:
        copy.start()
    barrier = pltpu.get_barrier_semaphore()
    for k in range(1, 16):
        pl.semaphore_signal(barrier, inc=1, device_id={"dp": (me + k) % 16}, device_id_type=MESH)
    pl.semaphore_wait(barrier, 15)

    sends = []
    for k in range(1, 16):
        copy = pltpu.make_async_remote_copy(
            sq, squares.at[me], sq_send.at[k], sq_recv.at[k], device_id={"dp": (me + k) % 16}, device_id_type=MESH
        )
        copy.start()
        sends.append(copy)
    squares[me] = sq[...]
    for copy in sends:
        copy.wait_recv()
    total = jnp.sum(jnp.sum(squares[...], axis=0), axis=(0, 1), keepdims=True)
    factor = jnp.minimum(1.0, 0.5 * lax.rsqrt(total / count + 1e-30))

    def ici(u, k, phase, i, l, cols):
        p, q, r = k, (k + 1) % 3, (k + 2) % 3
        where = list(at)
        for d in (p, q)[:phase]:
            where[d] = pl.ds(0, 2)
        there = new_w[i].at[l, where[0], where[1], where[2], core, :, pl.ds(*cols)]
        here = out_w[i].at[l, :, pl.ds(*cols)] if phase == 0 else there
        return pltpu.make_async_remote_copy(
            here,
            there,
            ici_send.at[3 * u + k, phase],
            ici_recv.at[3 * u + k, phase],
            device_id={"dp": flipped(me, LINKS[(p, q, r)[phase]])},
            device_id_type=MESH,
        )

    def d2d(u, k, piece, i, l, cols):
        order = (k, (k + 1) % 3, (k + 2) % 3)
        where = list(at)
        for d in order[: max(piece - 1, 0)]:
            where[d] = pl.ds(0, 2)
        if piece:
            where[order[piece - 1]] = 1 - at[order[piece - 1]]
        there = new_w[i].at[l, where[0], where[1], where[2], core, :, pl.ds(*cols)]
        here = out_w[i].at[l, :, pl.ds(*cols)] if piece == 0 else there
        return pltpu.make_async_remote_copy(
            here,
            there,
            d2d_send.at[3 * u + k, piece],
            d2d_recv.at[3 * u + k, piece],
            device_id={"dp": flipped(me, 1)},
            device_id_type=MESH,
        )

    moved, kept, stores = [], [], []
    for u, (i, l) in enumerate(units):
        loads[u].wait()
        clipped = g[i][l].astype(jnp.float32) * factor
        mm = 0.9 * m[i][l] + 0.1 * clipped
        vv = 0.95 * v[i][l] + 0.05 * clipped * clipped
        old = own_w[i][l].astype(jnp.float32)
        out_w[i][l] = (old - 0.02 * (mm * lax.rsqrt(vv + 1e-8) + 0.1 * old)).astype(jnp.bfloat16)
        out_m[i][l] = mm
        out_v[i][l] = vv
        for k, cols in enumerate(widths(shapes[i][2], u)):
            for copy in (ici(u, k, 0, i, l, cols), d2d(u, k, 0, i, l, cols)):
                copy.start()
                moved.append(copy)
        keep = pltpu.make_async_copy(out_w[i].at[l], new_w[i].at[l, at[0], at[1], at[2], core], keep_sem.at[u])
        keep.start()
        kept.append(keep)
        for j, (out, new) in enumerate(((out_m, new_m), (out_v, new_v))):
            store = pltpu.make_async_copy(out[i].at[l], new[i].at[l], mv_sem.at[u, j])
            store.start()
            stores.append(store)
    for keep in kept:
        keep.wait()
    for phase in range(3):
        for u, (i, l) in enumerate(units):
            for k, cols in enumerate(widths(shapes[i][2], u)):
                ici(u, k, phase, i, l, cols).wait_recv()
                follow = [d2d(u, k, phase + 1, i, l, cols)]
                if phase < 2:
                    follow.insert(0, ici(u, k, phase + 1, i, l, cols))
                for copy in follow:
                    copy.start()
                    moved.append(copy)
    for u, (i, l) in enumerate(units):
        for k, cols in enumerate(widths(shapes[i][2], u)):
            for piece in range(4):
                d2d(u, k, piece, i, l, cols).wait_recv()
    for copy in moved + sends:
        copy.wait_send()
    for store in stores:
        store.wait()


def step_and_gather(sq, g, w, m, v, count):
    shapes = [t.shape for t in m]
    n_units = sum(s[0] for s in shapes)
    blocks = [t.reshape(t.shape[0], 16, -1, t.shape[2]) for t in w]
    vmem, hbm = pl.BlockSpec(memory_space=pltpu.VMEM), pl.BlockSpec(memory_space=pl.ANY)
    dma = pltpu.SemaphoreType.DMA
    out = pl.pallas_call(
        functools.partial(gather_kernel, shapes, count),
        out_shape=[jax.ShapeDtypeStruct((s[0], 2, 2, 2, 2) + s[1:], jnp.bfloat16) for s in shapes]
        + [jax.ShapeDtypeStruct(s, jnp.float32) for s in shapes] * 2,
        in_specs=[vmem] + [vmem] * 3 + [hbm] * 3 + [vmem] * 6,
        out_specs=[hbm] * 9,
        scratch_shapes=[pltpu.VMEM(s, jnp.bfloat16) for s in shapes] * 2
        + [pltpu.VMEM(s, jnp.float32) for s in shapes] * 2
        + [
            pltpu.VMEM((16, 8, 128), jnp.float32),
            dma((16,)),
            dma((16,)),
            dma((n_units,)),
            dma((n_units,)),
            dma((n_units, 2)),
            dma((3 * n_units, 3)),
            dma((3 * n_units, 3)),
            dma((3 * n_units, 4)),
            dma((3 * n_units, 4)),
        ],
        compiler_params=pltpu.CompilerParams(collective_id=0, has_side_effects=True, vmem_limit_bytes=60 * 2**20),
        name="step_and_gather",
    )(sq, *g, *blocks, *m, *v)
    return [t.reshape(old.shape) for t, old in zip(out[:3], w)] + list(out[3:])


def solution(mesh):
    n = mesh.shape["dp"]

    def step(x, dy, w_gate, w_up, w_down, *moments):
        m, v = moments[:3], moments[3:]
        layers = w_gate.shape[0]
        h = x[0]
        saved = []
        for l in range(layers):
            wide = h.astype(jnp.float32)
            scale = lax.rsqrt(jnp.mean(wide**2, -1, keepdims=True) + 1e-6)
            a = (wide * scale).astype(jnp.bfloat16)
            gate = dot(a, w_gate[l], ((1,), (0,)))
            up = dot(a, w_up[l], ((1,), (0,)))
            z = (jax.nn.silu(gate) * up).astype(jnp.bfloat16)
            saved.append((h, scale, a, gate, up, z))
            if l + 1 < layers:
                h = h + dot(z, w_down[l], ((1,), (0,))).astype(jnp.bfloat16)
        d = dy[0]
        shards = {name: [None] * layers for name in NAMES}

        def scatter(t):
            return lax.psum_scatter(t.astype(jnp.bfloat16), "dp", scatter_dimension=0, tiled=True)

        for l in reversed(range(layers)):
            h, scale, a, gate, up, z = saved[l]
            shards["w_down"][l] = scatter(dot(z, d, ((0,), (0,))))
            dz = dot(d, w_down[l], ((1,), (1,))).astype(jnp.bfloat16).astype(jnp.float32)
            sig = jax.nn.sigmoid(gate)
            silu = gate * sig
            dup = (dz * silu).astype(jnp.bfloat16)
            dgate = (dz * up * (sig * (1 + gate * (1 - sig)))).astype(jnp.bfloat16)
            shards["w_gate"][l] = scatter(dot(a, dgate, ((0,), (0,))))
            shards["w_up"][l] = scatter(dot(a, dup, ((0,), (0,))))
            if l:
                da = dot(dgate, w_gate[l], ((1,), (1,))) + dot(dup, w_up[l], ((1,), (1,)))
                wide = h.astype(jnp.float32)
                back = da * scale - wide * (scale**3 * jnp.mean(da * wide, -1, keepdims=True))
                d = d + back.astype(jnp.bfloat16)

        g = [jnp.stack(shards[name]) for name in NAMES]
        part = sum(jnp.sum(jnp.square(t.astype(jnp.float32)).reshape(-1, 8, 128), axis=0) for t in g)
        return tuple(step_and_gather(part, g, (w_gate, w_up, w_down), m, v, sum(t.size for t in g) * n))

    seq, whole, rows = P(("rep", "dp"), None, None), P(), P(None, "dp", None)
    return jax.shard_map(
        step,
        mesh=mesh,
        in_specs=(seq, seq) + (whole,) * 3 + (rows,) * 6,
        out_specs=(P("rep", None, None),) * 3 + (P("rep", "dp", None),) * 6,
        check_vma=False,
    )
```

```python
import functools

import jax
import jax.numpy as jnp
from jax import lax
from jax.experimental import pallas as pl
from jax.experimental.pallas import tpu as pltpu
from jax.sharding import PartitionSpec as P

MESH = pl.DeviceIdType.MESH

NAMES = ("w_gate", "w_up", "w_down")


def dot(a, b, dims):
    return lax.dot_general(a, b, (dims, ((), ())), preferred_element_type=jnp.float32)


LINKS = (8, 4, 2)


def flipped(me, stride):
    return me + stride - 2 * stride * ((me // stride) % 2)


def widths(columns, turn):
    lanes = columns // 128
    sizes = [128 * ((lanes + (k + turn) % 3) // 3) for k in range(3)]
    starts = [0, sizes[0], sizes[0] + sizes[1]]
    return list(zip(starts, sizes))


def gather_kernel(shapes, count, sq, *refs):
    n_mat, layers, ff = len(shapes), shapes[0][0], shapes[0][2]
    gu, dn, refs = refs[:layers], refs[layers : 2 * layers], refs[2 * layers :]
    w, m, v, new_w, new_m, new_v, own_w, out_w, out_m, out_v = (refs[i * n_mat : (i + 1) * n_mat] for i in range(10))
    squares, sq_send, sq_recv, in_sem, keep_sem, mv_sem, ici_send, ici_recv, d2d_send, d2d_recv = refs[10 * n_mat :]
    me = lax.axis_index("dp")
    at = [(me // s) % 2 for s in LINKS]
    core = me % 2
    units = [(i, l) for l in reversed(range(shapes[0][0])) for i in range(n_mat)]

    loads = [pltpu.make_async_copy(w[i].at[l, me], own_w[i].at[l], in_sem.at[u]) for u, (i, l) in enumerate(units)]
    for copy in loads:
        copy.start()
    barrier = pltpu.get_barrier_semaphore()
    for k in range(1, 16):
        pl.semaphore_signal(barrier, inc=1, device_id={"dp": (me + k) % 16}, device_id_type=MESH)
    pl.semaphore_wait(barrier, 15)

    sends = []
    for k in range(1, 16):
        copy = pltpu.make_async_remote_copy(
            sq, squares.at[me], sq_send.at[k], sq_recv.at[k], device_id={"dp": (me + k) % 16}, device_id_type=MESH
        )
        copy.start()
        sends.append(copy)
    squares[me] = sq[...]
    for copy in sends:
        copy.wait_recv()
    total = jnp.sum(jnp.sum(squares[...], axis=0), axis=(0, 1), keepdims=True)
    factor = jnp.minimum(1.0, 0.5 * lax.rsqrt(total / count + 1e-30))

    def ici(u, k, phase, i, l, cols):
        p, q, r = k, (k + 1) % 3, (k + 2) % 3
        where = list(at)
        for d in (p, q)[:phase]:
            where[d] = pl.ds(0, 2)
        there = new_w[i].at[l, where[0], where[1], where[2], core, :, pl.ds(*cols)]
        here = out_w[i].at[l, :, pl.ds(*cols)] if phase == 0 else there
        return pltpu.make_async_remote_copy(
            here,
            there,
            ici_send.at[3 * u + k, phase],
            ici_recv.at[3 * u + k, phase],
            device_id={"dp": flipped(me, LINKS[(p, q, r)[phase]])},
            device_id_type=MESH,
        )

    def d2d(u, k, piece, i, l, cols):
        order = (k, (k + 1) % 3, (k + 2) % 3)
        where = list(at)
        for d in order[: max(piece - 1, 0)]:
            where[d] = pl.ds(0, 2)
        if piece:
            where[order[piece - 1]] = 1 - at[order[piece - 1]]
        there = new_w[i].at[l, where[0], where[1], where[2], core, :, pl.ds(*cols)]
        here = out_w[i].at[l, :, pl.ds(*cols)] if piece == 0 else there
        return pltpu.make_async_remote_copy(
            here,
            there,
            d2d_send.at[3 * u + k, piece],
            d2d_recv.at[3 * u + k, piece],
            device_id={"dp": flipped(me, 1)},
            device_id_type=MESH,
        )

    moved, kept, stores = [], [], []
    for u, (i, l) in enumerate(units):
        loads[u].wait()
        g = dn[l][...] if i == 2 else gu[l][:, i * ff : (i + 1) * ff]
        clipped = g.astype(jnp.float32) * factor
        mm = 0.9 * m[i][l] + 0.1 * clipped
        vv = 0.95 * v[i][l] + 0.05 * clipped * clipped
        old = own_w[i][l].astype(jnp.float32)
        out_w[i][l] = (old - 0.02 * (mm * lax.rsqrt(vv + 1e-8) + 0.1 * old)).astype(jnp.bfloat16)
        out_m[i][l] = mm
        out_v[i][l] = vv
        for k, cols in enumerate(widths(shapes[i][2], u)):
            for copy in (ici(u, k, 0, i, l, cols), d2d(u, k, 0, i, l, cols)):
                copy.start()
                moved.append(copy)
        keep = pltpu.make_async_copy(out_w[i].at[l], new_w[i].at[l, at[0], at[1], at[2], core], keep_sem.at[u])
        keep.start()
        kept.append(keep)
        for j, (out, new) in enumerate(((out_m, new_m), (out_v, new_v))):
            store = pltpu.make_async_copy(out[i].at[l], new[i].at[l], mv_sem.at[u, j])
            store.start()
            stores.append(store)
    for keep in kept:
        keep.wait()
    for phase in range(3):
        for u, (i, l) in enumerate(units):
            for k, cols in enumerate(widths(shapes[i][2], u)):
                ici(u, k, phase, i, l, cols).wait_recv()
                follow = [d2d(u, k, phase + 1, i, l, cols)]
                if phase < 2:
                    follow.insert(0, ici(u, k, phase + 1, i, l, cols))
                for copy in follow:
                    copy.start()
                    moved.append(copy)
    for u, (i, l) in enumerate(units):
        for k, cols in enumerate(widths(shapes[i][2], u)):
            for piece in range(4):
                d2d(u, k, piece, i, l, cols).wait_recv()
    for copy in moved + sends:
        copy.wait_send()
    for store in stores:
        store.wait()


def step_and_gather(sq, gu, dn, w, m, v, count):
    shapes = [t.shape for t in m]
    n_units = sum(s[0] for s in shapes)
    blocks = [t.reshape(t.shape[0], 16, -1, t.shape[2]) for t in w]
    vmem, hbm = pl.BlockSpec(memory_space=pltpu.VMEM), pl.BlockSpec(memory_space=pl.ANY)
    dma = pltpu.SemaphoreType.DMA
    out = pl.pallas_call(
        functools.partial(gather_kernel, shapes, count),
        out_shape=[jax.ShapeDtypeStruct((s[0], 2, 2, 2, 2) + s[1:], jnp.bfloat16) for s in shapes]
        + [jax.ShapeDtypeStruct(s, jnp.float32) for s in shapes] * 2,
        in_specs=[vmem] * (1 + len(gu) + len(dn)) + [hbm] * 3 + [vmem] * 6,
        out_specs=[hbm] * 9,
        scratch_shapes=[pltpu.VMEM(s, jnp.bfloat16) for s in shapes] * 2
        + [pltpu.VMEM(s, jnp.float32) for s in shapes] * 2
        + [
            pltpu.VMEM((16, 8, 128), jnp.float32),
            dma((16,)),
            dma((16,)),
            dma((n_units,)),
            dma((n_units,)),
            dma((n_units, 2)),
            dma((3 * n_units, 3)),
            dma((3 * n_units, 3)),
            dma((3 * n_units, 4)),
            dma((3 * n_units, 4)),
        ],
        compiler_params=pltpu.CompilerParams(collective_id=0, has_side_effects=True, vmem_limit_bytes=60 * 2**20),
        name="step_and_gather",
    )(sq, *gu, *dn, *blocks, *m, *v)
    return [t.reshape(old.shape) for t, old in zip(out[:3], w)] + list(out[3:])


UNIT = 256
LAGS = (2, 5, 8, 11)
DOWN_STEPS = (3, 9, 14, 18)


def fold(t):
    t = jnp.sum(jnp.square(t).reshape(-1, 8, t.shape[-1]), axis=0)
    return sum(t[:, j : j + 128] for j in range(0, t.shape[-1], 128))


def reduce_kernel(per, with_da, *refs):
    a_t, down, dgate, dup, *refs = refs
    if with_da:
        w_gate, w_up, *refs = refs
    gu, dn, sq, *refs = refs
    if with_da:
        da, *refs = refs
    tile, got, kept1, kept2, kept3, out1, out2, out3, in1, in2, in3 = refs[:11]
    d_own, d_got, d_kept1, d_kept2, d_kept3, d_out1, d_out2, d_out3, d_in1, d_in2, d_in3 = refs[11:22]
    stream, w_stream, s_sem, w_sem, send, recv, d_send, d_recv, own_sem = refs[22:]
    kept, outs, ins = (kept1, kept2, kept3), (out1, out2, out3), (in1, in2, in3)
    d_kept, d_outs, d_ins = (d_kept1, d_kept2, d_kept3), (d_out1, d_out2, d_out3), (d_in1, d_in2, d_in3)
    n_units = 2 * per
    me = lax.axis_index("dp")
    at = [(me // s) % 2 for s in LINKS]
    core = me % 2
    everything = slice(None)

    def remote(src, dst, s, r, stride):
        return pltpu.make_async_remote_copy(src, dst, s, r, device_id={"dp": flipped(me, stride)}, device_id_type=MESH)

    def hop(u, k, stage):
        if stage == 0:
            return remote(tile.at[u % 3, :, :, :, 1 - core], got.at[u], send.at[0, u], recv.at[0, u], 1)
        return remote(outs[stage - 1].at[u], ins[stage - 1].at[u], send.at[stage, u], recv.at[stage, u], LINKS[(k + stage - 1) % 3])

    def down_hop(k, stage):
        cols = pl.ds(*widths(dn.shape[1], 0)[k])
        if stage == 0:
            src, dst, stride = down.at[:, :, :, 1 - core, :, cols], d_got.at[:, :, :, :, cols], 1
        else:
            lead = (everything,) * (4 - stage)
            src, dst = d_outs[stage - 1].at[(*lead, cols)], d_ins[stage - 1].at[(*lead, cols)]
            stride = LINKS[(k + stage - 1) % 3]
        return remote(src, dst, d_send.at[stage, k], d_recv.at[stage, k], stride)

    def halves(k, stage):
        axes = [d for d in range(3) if d not in [(k + j) % 3 for j in range(stage - 1)]]
        d = (k + stage - 1) % 3
        return [tuple(side if axis == d else everything for axis in axes) for side in (1 - at[d], at[d])]

    def add_up(u, k, stage):
        hop(u, k, stage - 1).wait_recv()
        if stage == 1:
            hop(u, k, 0).wait_send()

        def total(where):
            if stage == 1:
                mine, other = tile[(u % 3, *where, core)], got[(u, *where)]
            else:
                mine, other = kept[stage - 2][(u % 4, *where)], ins[stage - 2][(u, *where)]
            return mine.astype(jnp.float32) + other.astype(jnp.float32)

        if stage == 4:
            g = total(()).astype(jnp.bfloat16)
            gu[:, pl.ds(pl.multiple_of(u * UNIT, UNIT), UNIT)] = g
            sq[...] += fold(g.astype(jnp.float32))
            return
        away, here = halves(k, stage)
        outs[stage - 1][u] = total(away).astype(jnp.bfloat16)
        hop(u, k, stage).start()
        kept[stage - 1][u % 4] = total(here)

    def add_down(k, stage):
        down_hop(k, stage - 1).wait_recv()
        cols = pl.ds(*widths(dn.shape[1], 0)[k])

        def total(where):
            mine, other = (d_own, d_got) if stage == 1 else (d_kept[stage - 2], d_ins[stage - 2])
            at_ = (*where, everything, cols)
            return mine[at_].astype(jnp.float32) + other[at_].astype(jnp.float32)

        if stage == 4:
            g = total(()).astype(jnp.bfloat16)
            dn[:, cols] = g
            sq[...] += fold(g.astype(jnp.float32))
            return
        away, here = halves(k, stage)
        rest = (everything,) * (4 - stage)
        d_outs[stage - 1][(*rest, cols)] = total(away).astype(jnp.bfloat16)
        down_hop(k, stage).start()
        d_kept[stage - 1][(*rest, cols)] = total(here)

    def loads(u, arrays):
        col = pl.ds(pl.multiple_of((u % per) * UNIT, UNIT), UNIT)
        slot = u % 2
        pairs = [(arrays[0], stream, s_sem)] + ([(arrays[1], w_stream, w_sem)] if with_da else [])
        return [pltpu.make_async_copy(src.at[:, col], dst.at[slot], sem.at[slot]) for src, dst, sem in pairs]

    def load(u):
        for which in range(2):

            @pl.when(u // per == which)
            def _():
                for copy in loads(u, ((dgate, dup)[which], (w_gate, w_up)[which] if with_da else None)):
                    copy.start()

    own = pltpu.make_async_copy(down.at[:, :, :, core], d_own, own_sem)
    own.start()
    load(0)
    barrier = pltpu.get_barrier_semaphore()
    for stride in (1, *LINKS):
        pl.semaphore_signal(barrier, inc=1, device_id={"dp": flipped(me, stride)}, device_id_type=MESH)
    pl.semaphore_wait(barrier, 4)
    for k in range(3):
        down_hop(k, 0).start()
    sq[...] = jnp.zeros_like(sq)
    if with_da:
        da[...] = jnp.zeros_like(da)
    own.wait()

    def step(t, _):
        @pl.when(t + 1 < n_units)
        def _():
            load(t + 1)

        for stage, lag in reversed(list(enumerate(LAGS, 1))):
            u = t - lag
            for k in range(3):

                @pl.when((u >= 0) & (u < n_units) & ((u + 33) % 3 == k))
                def _():
                    add_up(u, k, stage)

        for stage, when in enumerate(DOWN_STEPS, 1):

            @pl.when(t == when)
            def _():
                for k in range(3):
                    add_down(k, stage)

        @pl.when(t < n_units)
        def _():
            for copy in loads(t, (dgate, w_gate if with_da else None)):
                copy.wait()
            slot = t % 2
            g = jnp.dot(a_t[...], stream[slot], preferred_element_type=jnp.float32).astype(jnp.bfloat16)
            tile[t % 3] = g.reshape(tile.shape[1:])
            hop(t, 0, 0).start()
            if with_da:

                def rows(j, _):
                    part = pl.ds(pl.multiple_of(j * 512, 512), 512)
                    da[part] += lax.dot_general(
                        stream[slot, part], w_stream[slot], (((1,), (1,)), ((), ())), preferred_element_type=jnp.float32
                    )

                lax.fori_loop(0, da.shape[0] // 512, rows, None)

    lax.fori_loop(0, n_units + LAGS[-1], step, None)

    def drain(u, _):
        for stage in (1, 2, 3):
            hop(u, 0, stage).wait_send()

    lax.fori_loop(0, n_units, drain, None)
    for k in range(3):
        for stage in range(4):
            down_hop(k, stage).wait_send()


def reduce_layer(a, down, dgate, dup, weights, collective_id):
    tokens, d = a.shape
    ff = dgate.shape[1]
    per, rows, d_rows, with_da = ff // UNIT, d // 16, ff // 16, weights is not None
    n_units = 2 * per
    vmem, hbm = pl.BlockSpec(memory_space=pltpu.VMEM), pl.BlockSpec(memory_space=pl.ANY)
    dma, b16, f32 = pltpu.SemaphoreType.DMA, jnp.bfloat16, jnp.float32
    whole = [jax.ShapeDtypeStruct((tokens, d), f32)] if with_da else []
    return pl.pallas_call(
        functools.partial(reduce_kernel, per, with_da),
        out_shape=[
            jax.ShapeDtypeStruct((rows, 2 * ff), b16),
            jax.ShapeDtypeStruct((d_rows, d), b16),
            jax.ShapeDtypeStruct((8, 128), f32),
        ]
        + whole,
        in_specs=[vmem] + [hbm] * (5 if with_da else 3),
        out_specs=[vmem] * (3 + len(whole)),
        scratch_shapes=[
            pltpu.VMEM((3, 2, 2, 2, 2, rows, UNIT), b16),
            pltpu.VMEM((n_units, 2, 2, 2, rows, UNIT), b16),
            pltpu.VMEM((4, 2, 2, rows, UNIT), f32),
            pltpu.VMEM((4, 2, rows, UNIT), f32),
            pltpu.VMEM((4, rows, UNIT), f32),
        ]
        + [
            pltpu.VMEM((n_units, 2, 2, rows, UNIT), b16),
            pltpu.VMEM((n_units, 2, rows, UNIT), b16),
            pltpu.VMEM((n_units, rows, UNIT), b16),
        ]
        * 2
        + [pltpu.VMEM((2, 2, 2, d_rows, d), b16)] * 2
        + [pltpu.VMEM((2, 2, d_rows, d), f32), pltpu.VMEM((2, d_rows, d), f32), pltpu.VMEM((d_rows, d), f32)]
        + [pltpu.VMEM((2, 2, d_rows, d), b16), pltpu.VMEM((2, d_rows, d), b16), pltpu.VMEM((d_rows, d), b16)] * 2
        + [
            pltpu.VMEM((2, tokens, UNIT), b16),
            pltpu.VMEM((2, d, UNIT), b16),
            dma((2,)),
            dma((2,)),
            dma((4, n_units)),
            dma((4, n_units)),
            dma((4, 3)),
            dma((4, 3)),
            dma(()),
        ],
        compiler_params=pltpu.CompilerParams(collective_id=collective_id, has_side_effects=True, vmem_limit_bytes=62 * 2**20),
        name=f"reduce_layer_{collective_id}",
    )(a.T, down.reshape(2, 2, 2, 2, d_rows, d), dgate, dup, *(weights or ()))


def solution(mesh):
    n = mesh.shape["dp"]

    def step(x, dy, w_gate, w_up, w_down, *moments):
        m, v = moments[:3], moments[3:]
        layers = w_gate.shape[0]
        h = x[0]
        saved = []
        for l in range(layers):
            wide = h.astype(jnp.float32)
            scale = lax.rsqrt(jnp.mean(wide**2, -1, keepdims=True) + 1e-6)
            a = (wide * scale).astype(jnp.bfloat16)
            gate = dot(a, w_gate[l], ((1,), (0,)))
            up = dot(a, w_up[l], ((1,), (0,)))
            z = (jax.nn.silu(gate) * up).astype(jnp.bfloat16)
            saved.append((h, scale, a, gate, up, z))
            if l + 1 < layers:
                h = h + dot(z, w_down[l], ((1,), (0,))).astype(jnp.bfloat16)
        d = dy[0]
        summed, squares = [None] * layers, 0.0
        for l in reversed(range(layers)):
            h, scale, a, gate, up, z = saved[l]
            down = dot(z, d, ((0,), (0,))).astype(jnp.bfloat16)
            dz = dot(d, w_down[l], ((1,), (1,))).astype(jnp.bfloat16).astype(jnp.float32)
            sig = jax.nn.sigmoid(gate)
            silu = gate * sig
            dup = (dz * silu).astype(jnp.bfloat16)
            dgate = (dz * up * (sig * (1 + gate * (1 - sig)))).astype(jnp.bfloat16)
            gu, dn, sq, *da = reduce_layer(a, down, dgate, dup, (w_gate[l], w_up[l]) if l else None, l + 1)
            summed[l] = (gu, dn)
            squares = squares + sq
            if l:
                da = da[0]
                wide = h.astype(jnp.float32)
                back = da * scale - wide * (scale**3 * jnp.mean(da * wide, -1, keepdims=True))
                d = d + back.astype(jnp.bfloat16)

        gu, dn = zip(*summed, strict=True)
        count = sum(t.size for t in m) * n
        return tuple(step_and_gather(squares, gu, dn, (w_gate, w_up, w_down), m, v, count))

    seq, whole, rows = P(("rep", "dp"), None, None), P(), P(None, "dp", None)
    return jax.shard_map(
        step,
        mesh=mesh,
        in_specs=(seq, seq) + (whole,) * 3 + (rows,) * 6,
        out_specs=(P("rep", None, None),) * 3 + (P("rep", "dp", None),) * 6,
        check_vma=False,
    )
```

```python
import functools

import jax
import jax.numpy as jnp
from jax import lax
from jax.experimental import pallas as pl
from jax.experimental.pallas import tpu as pltpu
from jax.sharding import PartitionSpec as P

MESH = pl.DeviceIdType.MESH

NAMES = ("w_gate", "w_up", "w_down")


def dot(a, b, dims):
    return lax.dot_general(a, b, (dims, ((), ())), preferred_element_type=jnp.float32)


LINKS = (8, 4, 2)


def flipped(me, stride):
    return me + stride - 2 * stride * ((me // stride) % 2)


def widths(columns, turn):
    lanes = columns // 128
    sizes = [128 * ((lanes + (k + turn) % 3) // 3) for k in range(3)]
    starts = [0, sizes[0], sizes[0] + sizes[1]]
    return list(zip(starts, sizes))


def gather_kernel(shapes, count, sq, *refs):
    n_mat, layers, ff = len(shapes), shapes[0][0], shapes[0][2]
    gu, dn, refs = refs[:layers], refs[layers : 2 * layers], refs[2 * layers :]
    w, m, v, new_w, new_m, new_v, own_w, out_w, out_m, out_v = (refs[i * n_mat : (i + 1) * n_mat] for i in range(10))
    squares, sq_send, sq_recv, in_sem, keep_sem, mv_sem, ici_send, ici_recv, d2d_send, d2d_recv = refs[10 * n_mat :]
    me = lax.axis_index("dp")
    at = [(me // s) % 2 for s in LINKS]
    core = me % 2
    units = [(i, l) for l in reversed(range(shapes[0][0])) for i in range(n_mat)]

    loads = [pltpu.make_async_copy(w[i].at[l, me], own_w[i].at[l], in_sem.at[u]) for u, (i, l) in enumerate(units)]
    for copy in loads:
        copy.start()
    barrier = pltpu.get_barrier_semaphore()
    for k in range(1, 16):
        pl.semaphore_signal(barrier, inc=1, device_id={"dp": (me + k) % 16}, device_id_type=MESH)
    pl.semaphore_wait(barrier, 15)

    sends = []
    for k in range(1, 16):
        copy = pltpu.make_async_remote_copy(
            sq, squares.at[me], sq_send.at[k], sq_recv.at[k], device_id={"dp": (me + k) % 16}, device_id_type=MESH
        )
        copy.start()
        sends.append(copy)
    squares[me] = sq[...]
    for copy in sends:
        copy.wait_recv()
    total = jnp.sum(jnp.sum(squares[...], axis=0), axis=(0, 1), keepdims=True)
    factor = jnp.minimum(1.0, 0.5 * lax.rsqrt(total / count + 1e-30))

    def ici(u, k, phase, i, l, cols):
        p, q, r = k, (k + 1) % 3, (k + 2) % 3
        where = list(at)
        for d in (p, q)[:phase]:
            where[d] = pl.ds(0, 2)
        there = new_w[i].at[l, where[0], where[1], where[2], core, :, pl.ds(*cols)]
        here = out_w[i].at[l, :, pl.ds(*cols)] if phase == 0 else there
        return pltpu.make_async_remote_copy(
            here,
            there,
            ici_send.at[3 * u + k, phase],
            ici_recv.at[3 * u + k, phase],
            device_id={"dp": flipped(me, LINKS[(p, q, r)[phase]])},
            device_id_type=MESH,
        )

    def d2d(u, k, piece, i, l, cols):
        order = (k, (k + 1) % 3, (k + 2) % 3)
        where = list(at)
        for d in order[: max(piece - 1, 0)]:
            where[d] = pl.ds(0, 2)
        if piece:
            where[order[piece - 1]] = 1 - at[order[piece - 1]]
        there = new_w[i].at[l, where[0], where[1], where[2], core, :, pl.ds(*cols)]
        here = out_w[i].at[l, :, pl.ds(*cols)] if piece == 0 else there
        return pltpu.make_async_remote_copy(
            here,
            there,
            d2d_send.at[3 * u + k, piece],
            d2d_recv.at[3 * u + k, piece],
            device_id={"dp": flipped(me, 1)},
            device_id_type=MESH,
        )

    moved, kept, stores = [], [], []
    for u, (i, l) in enumerate(units):
        loads[u].wait()
        g = dn[l][...] if i == 2 else gu[l][:, i * ff : (i + 1) * ff]
        clipped = g.astype(jnp.float32) * factor
        mm = 0.9 * m[i][l] + 0.1 * clipped
        vv = 0.95 * v[i][l] + 0.05 * clipped * clipped
        old = own_w[i][l].astype(jnp.float32)
        out_w[i][l] = (old - 0.02 * (mm * lax.rsqrt(vv + 1e-8) + 0.1 * old)).astype(jnp.bfloat16)
        out_m[i][l] = mm
        out_v[i][l] = vv
        for k, cols in enumerate(widths(shapes[i][2], u)):
            for copy in (ici(u, k, 0, i, l, cols), d2d(u, k, 0, i, l, cols)):
                copy.start()
                moved.append(copy)
        keep = pltpu.make_async_copy(out_w[i].at[l], new_w[i].at[l, at[0], at[1], at[2], core], keep_sem.at[u])
        keep.start()
        kept.append(keep)
        for j, (out, new) in enumerate(((out_m, new_m), (out_v, new_v))):
            store = pltpu.make_async_copy(out[i].at[l], new[i].at[l], mv_sem.at[u, j])
            store.start()
            stores.append(store)
    for keep in kept:
        keep.wait()
    for phase in range(3):
        for u, (i, l) in enumerate(units):
            for k, cols in enumerate(widths(shapes[i][2], u)):
                ici(u, k, phase, i, l, cols).wait_recv()
                follow = [d2d(u, k, phase + 1, i, l, cols)]
                if phase < 2:
                    follow.insert(0, ici(u, k, phase + 1, i, l, cols))
                for copy in follow:
                    copy.start()
                    moved.append(copy)
    for u, (i, l) in enumerate(units):
        for k, cols in enumerate(widths(shapes[i][2], u)):
            for piece in range(4):
                d2d(u, k, piece, i, l, cols).wait_recv()
    for copy in moved + sends:
        copy.wait_send()
    for store in stores:
        store.wait()


def step_and_gather(sq, gu, dn, w, m, v, count):
    shapes = [t.shape for t in m]
    n_units = sum(s[0] for s in shapes)
    blocks = [t.reshape(t.shape[0], 16, -1, t.shape[2]) for t in w]
    vmem, hbm = pl.BlockSpec(memory_space=pltpu.VMEM), pl.BlockSpec(memory_space=pl.ANY)
    dma = pltpu.SemaphoreType.DMA
    out = pl.pallas_call(
        functools.partial(gather_kernel, shapes, count),
        out_shape=[jax.ShapeDtypeStruct((s[0], 2, 2, 2, 2) + s[1:], jnp.bfloat16) for s in shapes]
        + [jax.ShapeDtypeStruct(s, jnp.float32) for s in shapes] * 2,
        in_specs=[vmem] * (1 + len(gu) + len(dn)) + [hbm] * 3 + [vmem] * 6,
        out_specs=[hbm] * 9,
        scratch_shapes=[pltpu.VMEM(s, jnp.bfloat16) for s in shapes] * 2
        + [pltpu.VMEM(s, jnp.float32) for s in shapes] * 2
        + [
            pltpu.VMEM((16, 8, 128), jnp.float32),
            dma((16,)),
            dma((16,)),
            dma((n_units,)),
            dma((n_units,)),
            dma((n_units, 2)),
            dma((3 * n_units, 3)),
            dma((3 * n_units, 3)),
            dma((3 * n_units, 4)),
            dma((3 * n_units, 4)),
        ],
        compiler_params=pltpu.CompilerParams(collective_id=0, has_side_effects=True, vmem_limit_bytes=60 * 2**20),
        name="step_and_gather",
    )(sq, *gu, *dn, *blocks, *m, *v)
    return [t.reshape(old.shape) for t, old in zip(out[:3], w)] + list(out[3:])


UNIT = 256
LAGS = (2, 5, 8, 11)
DOWN_STEPS = (3, 9, 14, 18)


def fold(t):
    t = jnp.sum(jnp.square(t).reshape(-1, 8, t.shape[-1]), axis=0)
    return sum(t[:, j : j + 128] for j in range(0, t.shape[-1], 128))


def reduce_kernel(per, l, with_da, *refs):
    a_t, d, down, gate, up, w_down, *refs = refs
    if with_da:
        w_gate, w_up, h, *refs = refs
    gu, dn, sq, *refs = refs
    if with_da:
        new_d, *refs = refs
    tile, got, kept1, kept2, kept3, out1, out2, out3, in1, in2, in3 = refs[:11]
    d_own, d_got, d_kept1, d_kept2, d_kept3, d_out1, d_out2, d_out3, d_in1, d_in2, d_in3 = refs[11:22]
    gates, ups, d_gu, wd, p_sem, w_sem, send, recv, d_send, d_recv, own_sem, *refs = refs[22:]
    if with_da:
        da, wgu, h_part, h_sem = refs
    kept, outs, ins = (kept1, kept2, kept3), (out1, out2, out3), (in1, in2, in3)
    d_kept, d_outs, d_ins = (d_kept1, d_kept2, d_kept3), (d_out1, d_out2, d_out3), (d_in1, d_in2, d_in3)
    n_units = 2 * per
    me = lax.axis_index("dp")
    at = [(me // s) % 2 for s in LINKS]
    core = me % 2
    everything = slice(None)
    part = gates.shape[1]
    parts = d.shape[0] // part

    def remote(src, dst, s, r, stride):
        return pltpu.make_async_remote_copy(src, dst, s, r, device_id={"dp": flipped(me, stride)}, device_id_type=MESH)

    def hop(u, k, stage):
        if stage == 0:
            return remote(tile.at[u % 3, :, :, :, 1 - core], got.at[u % 4], send.at[0, u], recv.at[0, u], 1)
        return remote(outs[stage - 1].at[u], ins[stage - 1].at[u % 6], send.at[stage, u], recv.at[stage, u], LINKS[(k + stage - 1) % 3])

    def down_hop(k, stage):
        cols = pl.ds(*widths(dn.shape[1], 0)[k])
        if stage == 0:
            src, dst, stride = down.at[:, :, :, 1 - core, :, cols], d_got.at[:, :, :, :, cols], 1
        else:
            lead = (everything,) * (4 - stage)
            src, dst = d_outs[stage - 1].at[(*lead, cols)], d_ins[stage - 1].at[(*lead, cols)]
            stride = LINKS[(k + stage - 1) % 3]
        return remote(src, dst, d_send.at[stage, k], d_recv.at[stage, k], stride)

    def halves(k, stage):
        axes = [d for d in range(3) if d not in [(k + j) % 3 for j in range(stage - 1)]]
        d = (k + stage - 1) % 3
        return [tuple(side if axis == d else everything for axis in axes) for side in (1 - at[d], at[d])]

    def add_up(u, k, stage):
        hop(u, k, stage - 1).wait_recv()
        if stage == 1:
            hop(u, k, 0).wait_send()

        def total(where):
            if stage == 1:
                mine, other = tile[(u % 3, *where, core)], got[(u % 4, *where)]
            else:
                mine, other = kept[stage - 2][(u % 4, *where)], ins[stage - 2][(u % 6, *where)]
            return mine.astype(jnp.float32) + other.astype(jnp.float32)

        if stage == 4:
            g = total(()).astype(jnp.bfloat16)
            gu[:, pl.ds(pl.multiple_of((u % 2) * per * UNIT + (u // 2) * UNIT, UNIT), UNIT)] = g
            sq[...] += fold(g.astype(jnp.float32))
            return
        away, here = halves(k, stage)
        outs[stage - 1][u] = total(away).astype(jnp.bfloat16)
        hop(u, k, stage).start()
        kept[stage - 1][u % 4] = total(here)

    def add_down(k, stage):
        down_hop(k, stage - 1).wait_recv()
        cols = pl.ds(*widths(dn.shape[1], 0)[k])

        def total(where):
            mine, other = (d_own, d_got) if stage == 1 else (d_kept[stage - 2], d_ins[stage - 2])
            at_ = (*where, everything, cols)
            return mine[at_].astype(jnp.float32) + other[at_].astype(jnp.float32)

        if stage == 4:
            g = total(()).astype(jnp.bfloat16)
            dn[:, cols] = g
            sq[...] += fold(g.astype(jnp.float32))
            return
        away, here = halves(k, stage)
        rest = (everything,) * (4 - stage)
        d_outs[stage - 1][(*rest, cols)] = total(away).astype(jnp.bfloat16)
        down_hop(k, stage).start()
        d_kept[stage - 1][(*rest, cols)] = total(here)

    def chunk(j):
        return pl.ds(pl.multiple_of(j * UNIT, UNIT), UNIT)

    def part_loads(j, p):
        rows = pl.ds(pl.multiple_of(p * part, part), part)
        pairs = ((gate, gates), (up, ups))
        return [pltpu.make_async_copy(s.at[rows, chunk(j)], t.at[p], p_sem.at[i, p]) for i, (s, t) in enumerate(pairs)]

    def weight_loads(j):
        slot = j % 2
        copies = [pltpu.make_async_copy(w_down.at[l, chunk(j)], wd.at[slot], w_sem.at[0, slot])]
        if with_da:
            for i, w in enumerate((w_gate, w_up)):
                copies.append(pltpu.make_async_copy(w.at[l, :, chunk(j)], wgu.at[slot, i], w_sem.at[1 + i, slot]))
        return copies

    def start(copies):
        for copy in copies:
            copy.start()

    def back_through(j):
        for copy in weight_loads(j):
            copy.wait()

        @pl.when(j + 1 < per)
        def _():
            start(weight_loads(j + 1))

        slot = j % 2

        def one(p, _):
            for copy in part_loads(j, p):
                copy.wait()
            rows = pl.ds(pl.multiple_of(p * part, part), part)
            dz = lax.dot_general(d[rows], wd[slot], (((1,), (1,)), ((), ())), preferred_element_type=jnp.float32)
            dz = dz.astype(jnp.bfloat16).astype(jnp.float32)
            g, u = gates[p], ups[p]
            sig = jax.nn.sigmoid(g)
            d_u = (dz * (g * sig)).astype(jnp.bfloat16)
            d_g = (dz * u * (sig * (1 + g * (1 - sig)))).astype(jnp.bfloat16)
            d_gu[0, rows] = d_g
            d_gu[1, rows] = d_u
            if with_da:
                da[rows] += lax.dot_general(
                    d_g, wgu[slot, 0], (((1,), (1,)), ((), ())), preferred_element_type=jnp.float32
                ) + lax.dot_general(d_u, wgu[slot, 1], (((1,), (1,)), ((), ())), preferred_element_type=jnp.float32)

            @pl.when(j + 1 < per)
            def _():
                start(part_loads(j + 1, p))

        lax.fori_loop(0, parts, one, None)

    def h_load(p):
        rows = pl.ds(pl.multiple_of(p * part, part), part)
        return pltpu.make_async_copy(h.at[rows], h_part.at[p % 2], h_sem.at[0, p % 2])

    def d_store(p):
        rows = pl.ds(pl.multiple_of(p * part, part), part)
        return pltpu.make_async_copy(h_part.at[p % 2], new_d.at[rows], h_sem.at[1, p % 2])

    def norm_back(p):
        h_load(p).wait()
        rows = pl.ds(pl.multiple_of(p * part, part), part)
        wide = h_part[p % 2].astype(jnp.float32)
        scale = lax.rsqrt(jnp.mean(wide * wide, -1, keepdims=True) + 1e-6)
        grad = da[rows]
        back = grad * scale - wide * (scale * scale * scale * jnp.mean(grad * wide, -1, keepdims=True))
        total = d[rows].astype(jnp.float32) + back.astype(jnp.bfloat16).astype(jnp.float32)
        h_part[p % 2] = total.astype(jnp.bfloat16)
        d_store(p).start()

        @pl.when(p + 2 < parts)
        def _():
            d_store(p).wait()
            h_load(p + 2).start()

    own = pltpu.make_async_copy(down.at[:, :, :, core], d_own, own_sem)
    own.start()
    start(weight_loads(0))
    for p in range(parts):
        start(part_loads(0, p))
    barrier = pltpu.get_barrier_semaphore()
    for stride in (1, *LINKS):
        pl.semaphore_signal(barrier, inc=1, device_id={"dp": flipped(me, stride)}, device_id_type=MESH)
    pl.semaphore_wait(barrier, 4)
    for k in range(3):
        down_hop(k, 0).start()
    sq[...] = jnp.zeros_like(sq)
    if with_da:
        da[...] = jnp.zeros_like(da)
    own.wait()

    def step(t, _):
        for stage, lag in reversed(list(enumerate(LAGS, 1))):
            u = t - lag
            for k in range(3):

                @pl.when((u >= 0) & (u < n_units) & ((u + 33) % 3 == k))
                def _():
                    add_up(u, k, stage)

        for stage, when in enumerate(DOWN_STEPS, 1):

            @pl.when(t == when)
            def _():
                for k in range(3):
                    add_down(k, stage)

        @pl.when(t < n_units)
        def _():
            @pl.when(t % 2 == 0)
            def _():
                back_through(t // 2)

            g = jnp.dot(a_t[...], d_gu[t % 2], preferred_element_type=jnp.float32).astype(jnp.bfloat16)
            tile[t % 3] = g.reshape(tile.shape[1:])
            hop(t, 0, 0).start()

        if with_da:

            @pl.when(t == n_units - 1)
            def _():
                for p in range(2):
                    h_load(p).start()

            @pl.when((t >= n_units) & (t < n_units + parts))
            def _():
                norm_back(t - n_units)

    lax.fori_loop(0, n_units + LAGS[-1], step, None)

    def drain(u, _):
        for stage in (1, 2, 3):
            hop(u, 0, stage).wait_send()

    lax.fori_loop(0, n_units, drain, None)
    for k in range(3):
        for stage in range(4):
            down_hop(k, stage).wait_send()
    if with_da:
        for p in (parts - 2, parts - 1):
            d_store(p).wait()


def reduce_layer(a, d, down, gate, up, w_down, l, h, weights, collective_id):
    tokens, width = a.shape
    ff = gate.shape[1]
    per, rows, d_rows, with_da = ff // UNIT, width // 16, ff // 16, weights is not None
    n_units, part = 2 * per, tokens // 4
    vmem, hbm = pl.BlockSpec(memory_space=pltpu.VMEM), pl.BlockSpec(memory_space=pl.ANY)
    dma, b16, f32 = pltpu.SemaphoreType.DMA, jnp.bfloat16, jnp.float32
    return pl.pallas_call(
        functools.partial(reduce_kernel, per, l, with_da),
        out_shape=[
            jax.ShapeDtypeStruct((rows, 2 * ff), b16),
            jax.ShapeDtypeStruct((d_rows, width), b16),
            jax.ShapeDtypeStruct((8, 128), f32),
        ]
        + [jax.ShapeDtypeStruct((tokens, width), b16)] * with_da,
        in_specs=[vmem] * 2 + [hbm] * (7 if with_da else 4),
        out_specs=[vmem] * 3 + [hbm] * with_da,
        scratch_shapes=[
            pltpu.VMEM((3, 2, 2, 2, 2, rows, UNIT), b16),
            pltpu.VMEM((4, 2, 2, 2, rows, UNIT), b16),
            pltpu.VMEM((4, 2, 2, rows, UNIT), f32),
            pltpu.VMEM((4, 2, rows, UNIT), f32),
            pltpu.VMEM((4, rows, UNIT), f32),
        ]
        + [pltpu.VMEM((slots, *lead, rows, UNIT), b16) for slots in (n_units, 6) for lead in ((2, 2), (2,), ())]
        + [pltpu.VMEM((2, 2, 2, d_rows, width), b16)] * 2
        + [pltpu.VMEM((2, 2, d_rows, width), f32), pltpu.VMEM((2, d_rows, width), f32), pltpu.VMEM((d_rows, width), f32)]
        + [pltpu.VMEM((2, 2, d_rows, width), b16), pltpu.VMEM((2, d_rows, width), b16), pltpu.VMEM((d_rows, width), b16)] * 2
        + [pltpu.VMEM((4, part, UNIT), f32)] * 2
        + [
            pltpu.VMEM((2, tokens, UNIT), b16),
            pltpu.VMEM((2, UNIT, width), b16),
            dma((2, 4)),
            dma((3, 2)),
            dma((4, n_units)),
            dma((4, n_units)),
            dma((4, 3)),
            dma((4, 3)),
            dma(()),
        ]
        + [
            pltpu.VMEM((tokens, width), f32),
            pltpu.VMEM((2, 2, width, UNIT), b16),
            pltpu.VMEM((2, part, width), b16),
            dma((2, 2)),
        ]
        * with_da,
        compiler_params=pltpu.CompilerParams(collective_id=collective_id, has_side_effects=True, vmem_limit_bytes=63 * 2**20),
        name=f"reduce_layer_{collective_id}",
    )(a.T, d, down.reshape(2, 2, 2, 2, d_rows, width), gate, up, w_down, *((*weights, h) if with_da else ()))


def solution(mesh):
    n = mesh.shape["dp"]

    def step(x, dy, w_gate, w_up, w_down, *moments):
        m, v = moments[:3], moments[3:]
        layers = w_gate.shape[0]
        h = x[0]
        saved = []
        for l in range(layers):
            wide = h.astype(jnp.float32)
            scale = lax.rsqrt(jnp.mean(wide**2, -1, keepdims=True) + 1e-6)
            a = (wide * scale).astype(jnp.bfloat16)
            gate = dot(a, w_gate[l], ((1,), (0,)))
            up = dot(a, w_up[l], ((1,), (0,)))
            z = (jax.nn.silu(gate) * up).astype(jnp.bfloat16)
            saved.append((h, scale, a, gate, up, z))
            if l + 1 < layers:
                h = h + dot(z, w_down[l], ((1,), (0,))).astype(jnp.bfloat16)
        d = dy[0]
        summed, squares = [None] * layers, 0.0
        for l in reversed(range(layers)):
            h, scale, a, gate, up, z = saved[l]
            down = dot(z, d, ((0,), (0,))).astype(jnp.bfloat16)
            weights = (w_gate, w_up) if l else None
            gu, dn, sq, *new_d = reduce_layer(a, d, down, gate, up, w_down, l, h, weights, l + 1)
            summed[l] = (gu, dn)
            squares = squares + sq
            if l:
                d = new_d[0]

        gu, dn = zip(*summed, strict=True)
        count = sum(t.size for t in m) * n
        return tuple(step_and_gather(squares, gu, dn, (w_gate, w_up, w_down), m, v, count))

    seq, whole, rows = P(("rep", "dp"), None, None), P(), P(None, "dp", None)
    return jax.shard_map(
        step,
        mesh=mesh,
        in_specs=(seq, seq) + (whole,) * 3 + (rows,) * 6,
        out_specs=(P("rep", None, None),) * 3 + (P("rep", "dp", None),) * 6,
        check_vma=False,
    )
```

```python
import functools

import jax
import jax.numpy as jnp
from jax import lax
from jax.experimental import pallas as pl
from jax.experimental.pallas import tpu as pltpu
from jax.sharding import PartitionSpec as P

MESH = pl.DeviceIdType.MESH

NAMES = ("w_gate", "w_up", "w_down")


def dot(a, b, dims):
    return lax.dot_general(a, b, (dims, ((), ())), preferred_element_type=jnp.float32)


LINKS = (8, 4, 2)


def flipped(me, stride):
    return me + stride - 2 * stride * ((me // stride) % 2)


def widths(columns, turn):
    lanes = columns // 128
    sizes = [128 * ((lanes + (k + turn) % 3) // 3) for k in range(3)]
    starts = [0, sizes[0], sizes[0] + sizes[1]]
    return list(zip(starts, sizes))


def gather_kernel(shapes, count, sq, *refs):
    n_mat, layers, ff = len(shapes), shapes[0][0], shapes[0][2]
    gu, dn, refs = refs[:layers], refs[layers : 2 * layers], refs[2 * layers :]
    w, m, v, new_w, new_m, new_v, own_w, out_w, out_m, out_v = (refs[i * n_mat : (i + 1) * n_mat] for i in range(10))
    squares, sq_send, sq_recv, in_sem, keep_sem, mv_sem, ici_send, ici_recv, d2d_send, d2d_recv = refs[10 * n_mat :]
    me = lax.axis_index("dp")
    at = [(me // s) % 2 for s in LINKS]
    core = me % 2
    units = [(i, l) for l in reversed(range(shapes[0][0])) for i in range(n_mat)]

    loads = [pltpu.make_async_copy(w[i].at[l, me], own_w[i].at[l], in_sem.at[u]) for u, (i, l) in enumerate(units)]
    for copy in loads:
        copy.start()
    barrier = pltpu.get_barrier_semaphore()
    for k in range(1, 16):
        pl.semaphore_signal(barrier, inc=1, device_id={"dp": (me + k) % 16}, device_id_type=MESH)
    pl.semaphore_wait(barrier, 15)

    sends = []
    for k in range(1, 16):
        copy = pltpu.make_async_remote_copy(
            sq, squares.at[me], sq_send.at[k], sq_recv.at[k], device_id={"dp": (me + k) % 16}, device_id_type=MESH
        )
        copy.start()
        sends.append(copy)
    squares[me] = sq[...]
    for copy in sends:
        copy.wait_recv()
    total = jnp.sum(jnp.sum(squares[...], axis=0), axis=(0, 1), keepdims=True)
    factor = jnp.minimum(1.0, 0.5 * lax.rsqrt(total / count + 1e-30))

    def ici(u, k, phase, i, l, cols):
        p, q, r = k, (k + 1) % 3, (k + 2) % 3
        where = list(at)
        for d in (p, q)[:phase]:
            where[d] = pl.ds(0, 2)
        there = new_w[i].at[l, where[0], where[1], where[2], core, :, pl.ds(*cols)]
        here = out_w[i].at[l, :, pl.ds(*cols)] if phase == 0 else there
        return pltpu.make_async_remote_copy(
            here,
            there,
            ici_send.at[3 * u + k, phase],
            ici_recv.at[3 * u + k, phase],
            device_id={"dp": flipped(me, LINKS[(p, q, r)[phase]])},
            device_id_type=MESH,
        )

    def d2d(u, k, piece, i, l, cols):
        order = (k, (k + 1) % 3, (k + 2) % 3)
        where = list(at)
        for d in order[: max(piece - 1, 0)]:
            where[d] = pl.ds(0, 2)
        if piece:
            where[order[piece - 1]] = 1 - at[order[piece - 1]]
        there = new_w[i].at[l, where[0], where[1], where[2], core, :, pl.ds(*cols)]
        here = out_w[i].at[l, :, pl.ds(*cols)] if piece == 0 else there
        return pltpu.make_async_remote_copy(
            here,
            there,
            d2d_send.at[3 * u + k, piece],
            d2d_recv.at[3 * u + k, piece],
            device_id={"dp": flipped(me, 1)},
            device_id_type=MESH,
        )

    moved, kept, stores = [], [], []
    for u, (i, l) in enumerate(units):
        loads[u].wait()
        g = dn[l][...] if i == 2 else gu[l][:, i * ff : (i + 1) * ff]
        clipped = g.astype(jnp.float32) * factor
        mm = 0.9 * m[i][l] + 0.1 * clipped
        vv = 0.95 * v[i][l] + 0.05 * clipped * clipped
        old = own_w[i][l].astype(jnp.float32)
        out_w[i][l] = (old - 0.02 * (mm * lax.rsqrt(vv + 1e-8) + 0.1 * old)).astype(jnp.bfloat16)
        out_m[i][l] = mm
        out_v[i][l] = vv
        for k, cols in enumerate(widths(shapes[i][2], u)):
            for copy in (ici(u, k, 0, i, l, cols), d2d(u, k, 0, i, l, cols)):
                copy.start()
                moved.append(copy)
        keep = pltpu.make_async_copy(out_w[i].at[l], new_w[i].at[l, at[0], at[1], at[2], core], keep_sem.at[u])
        keep.start()
        kept.append(keep)
        for j, (out, new) in enumerate(((out_m, new_m), (out_v, new_v))):
            store = pltpu.make_async_copy(out[i].at[l], new[i].at[l], mv_sem.at[u, j])
            store.start()
            stores.append(store)
    for keep in kept:
        keep.wait()
    for phase in range(3):
        for u, (i, l) in enumerate(units):
            for k, cols in enumerate(widths(shapes[i][2], u)):
                ici(u, k, phase, i, l, cols).wait_recv()
                follow = [d2d(u, k, phase + 1, i, l, cols)]
                if phase < 2:
                    follow.insert(0, ici(u, k, phase + 1, i, l, cols))
                for copy in follow:
                    copy.start()
                    moved.append(copy)
    for u, (i, l) in enumerate(units):
        for k, cols in enumerate(widths(shapes[i][2], u)):
            for piece in range(4):
                d2d(u, k, piece, i, l, cols).wait_recv()
    for copy in moved + sends:
        copy.wait_send()
    for store in stores:
        store.wait()


def step_and_gather(sq, gu, dn, w, m, v, count):
    shapes = [t.shape for t in m]
    n_units = sum(s[0] for s in shapes)
    blocks = [t.reshape(t.shape[0], 16, -1, t.shape[2]) for t in w]
    vmem, hbm = pl.BlockSpec(memory_space=pltpu.VMEM), pl.BlockSpec(memory_space=pl.ANY)
    dma = pltpu.SemaphoreType.DMA
    out = pl.pallas_call(
        functools.partial(gather_kernel, shapes, count),
        out_shape=[jax.ShapeDtypeStruct((s[0], 2, 2, 2, 2) + s[1:], jnp.bfloat16) for s in shapes]
        + [jax.ShapeDtypeStruct(s, jnp.float32) for s in shapes] * 2,
        in_specs=[vmem] * (1 + len(gu) + len(dn)) + [hbm] * 3 + [vmem] * 6,
        out_specs=[hbm] * 9,
        scratch_shapes=[pltpu.VMEM(s, jnp.bfloat16) for s in shapes] * 2
        + [pltpu.VMEM(s, jnp.float32) for s in shapes] * 2
        + [
            pltpu.VMEM((16, 8, 128), jnp.float32),
            dma((16,)),
            dma((16,)),
            dma((n_units,)),
            dma((n_units,)),
            dma((n_units, 2)),
            dma((3 * n_units, 3)),
            dma((3 * n_units, 3)),
            dma((3 * n_units, 4)),
            dma((3 * n_units, 4)),
        ],
        compiler_params=pltpu.CompilerParams(collective_id=0, has_side_effects=True, vmem_limit_bytes=60 * 2**20),
        name="step_and_gather",
    )(sq, *gu, *dn, *blocks, *m, *v)
    return [t.reshape(old.shape) for t, old in zip(out[:3], w)] + list(out[3:])


UNIT = 256
LAGS = (2, 5, 8, 11)
DOWN_STEPS = (3, 9, 14, 18)


def forward_kernel(last, h, w_gate, w_up, *refs):
    if last:
        gate, up, z_t, a_t, a = refs
    else:
        w_down, gate, up, z_t, a_t, new_h, a, total = refs
    j, part = pl.program_id(0), h.shape[0] // 4

    def over_parts(body):
        lax.fori_loop(0, 4, lambda p, _: body(pl.ds(pl.multiple_of(p * part, part), part)), None)

    @pl.when(j == 0)
    def _():
        def norm(rows):
            wide = h[rows].astype(jnp.float32)
            scale = lax.rsqrt(jnp.mean(wide * wide, -1, keepdims=True) + 1e-6)
            a[rows] = (wide * scale).astype(jnp.bfloat16)
            a_t[:, rows] = a[rows].T
            if not last:
                total[rows] = jnp.zeros((part, total.shape[1]), jnp.float32)

        over_parts(norm)

    def hidden(rows):
        g = jnp.dot(a[rows], w_gate[...], preferred_element_type=jnp.float32)
        u = jnp.dot(a[rows], w_up[...], preferred_element_type=jnp.float32)
        gate[rows] = g
        up[rows] = u
        z = (jax.nn.silu(g) * u).astype(jnp.bfloat16)
        z_t[:, rows] = z.T
        if not last:
            total[rows] += jnp.dot(z, w_down[...], preferred_element_type=jnp.float32)

    over_parts(hidden)
    if not last:

        @pl.when(j == pl.num_programs(0) - 1)
        def _():
            def leave(rows):
                new_h[rows] = (h[rows].astype(jnp.float32) + total[rows].astype(jnp.bfloat16).astype(jnp.float32)).astype(jnp.bfloat16)

            over_parts(leave)


def forward_layer(h, w_gate, w_up, w_down, l, last):
    tokens, d = h.shape
    ff = w_gate.shape[2]
    b16, f32 = jnp.bfloat16, jnp.float32
    whole = lambda shape: pl.BlockSpec(shape, lambda j: (0, 0))
    column = pl.BlockSpec((None, d, UNIT), lambda j: (l, 0, j))
    hidden = pl.BlockSpec((tokens, UNIT), lambda j: (0, j))
    return pl.pallas_call(
        functools.partial(forward_kernel, last),
        grid=(ff // UNIT,),
        out_shape=[jax.ShapeDtypeStruct((tokens, ff), f32)] * 2
        + [jax.ShapeDtypeStruct((ff, tokens), b16), jax.ShapeDtypeStruct((d, tokens), b16)]
        + [jax.ShapeDtypeStruct((tokens, d), b16)] * (not last),
        in_specs=[whole((tokens, d)), column, column]
        + [pl.BlockSpec((None, UNIT, d), lambda j: (l, j, 0))] * (not last),
        out_specs=[hidden, hidden, pl.BlockSpec((UNIT, tokens), lambda j: (j, 0)), whole((d, tokens))]
        + [whole((tokens, d))] * (not last),
        scratch_shapes=[pltpu.VMEM((tokens, d), b16)] + [pltpu.VMEM((tokens, d), f32)] * (not last),
        compiler_params=pltpu.CompilerParams(dimension_semantics=("arbitrary",), vmem_limit_bytes=60 * 2**20),
        name=f"forward_layer_{l}",
    )(h, w_gate, w_up, *(() if last else (w_down,)))


def fold(t):
    t = jnp.sum(jnp.square(t).reshape(-1, 8, t.shape[-1]), axis=0)
    return sum(t[:, j : j + 128] for j in range(0, t.shape[-1], 128))


def reduce_kernel(per, l, with_da, *refs):
    a_t, d, down, gate, up, w_down, *refs = refs
    if with_da:
        w_gate, w_up, h, *refs = refs
    gu, dn, sq, *refs = refs
    if with_da:
        new_d, *refs = refs
    tile, got, kept1, kept2, kept3, out1, out2, out3, in1, in2, in3 = refs[:11]
    d_own, d_got, d_kept1, d_kept2, d_kept3, d_out1, d_out2, d_out3, d_in1, d_in2, d_in3 = refs[11:22]
    gates, ups, d_gu, wd, p_sem, w_sem, send, recv, d_send, d_recv, own_sem, *refs = refs[22:]
    if with_da:
        da, wgu, h_part, h_sem = refs
    kept, outs, ins = (kept1, kept2, kept3), (out1, out2, out3), (in1, in2, in3)
    d_kept, d_outs, d_ins = (d_kept1, d_kept2, d_kept3), (d_out1, d_out2, d_out3), (d_in1, d_in2, d_in3)
    n_units = 2 * per
    me = lax.axis_index("dp")
    at = [(me // s) % 2 for s in LINKS]
    core = me % 2
    everything = slice(None)
    part = gates.shape[1]
    parts = d.shape[0] // part

    def remote(src, dst, s, r, stride):
        return pltpu.make_async_remote_copy(src, dst, s, r, device_id={"dp": flipped(me, stride)}, device_id_type=MESH)

    def hop(u, k, stage):
        if stage == 0:
            return remote(tile.at[u % 3, :, :, :, 1 - core], got.at[u % 4], send.at[0, u], recv.at[0, u], 1)
        return remote(outs[stage - 1].at[u], ins[stage - 1].at[u % 6], send.at[stage, u], recv.at[stage, u], LINKS[(k + stage - 1) % 3])

    def down_hop(k, stage):
        cols = pl.ds(*widths(dn.shape[1], 0)[k])
        if stage == 0:
            src, dst, stride = down.at[:, :, :, 1 - core, :, cols], d_got.at[:, :, :, :, cols], 1
        else:
            lead = (everything,) * (4 - stage)
            src, dst = d_outs[stage - 1].at[(*lead, cols)], d_ins[stage - 1].at[(*lead, cols)]
            stride = LINKS[(k + stage - 1) % 3]
        return remote(src, dst, d_send.at[stage, k], d_recv.at[stage, k], stride)

    def halves(k, stage):
        axes = [d for d in range(3) if d not in [(k + j) % 3 for j in range(stage - 1)]]
        d = (k + stage - 1) % 3
        return [tuple(side if axis == d else everything for axis in axes) for side in (1 - at[d], at[d])]

    def add_up(u, k, stage):
        hop(u, k, stage - 1).wait_recv()
        if stage == 1:
            hop(u, k, 0).wait_send()

        def total(where):
            if stage == 1:
                mine, other = tile[(u % 3, *where, core)], got[(u % 4, *where)]
            else:
                mine, other = kept[stage - 2][(u % 4, *where)], ins[stage - 2][(u % 6, *where)]
            return mine.astype(jnp.float32) + other.astype(jnp.float32)

        if stage == 4:
            g = total(()).astype(jnp.bfloat16)
            gu[:, pl.ds(pl.multiple_of((u % 2) * per * UNIT + (u // 2) * UNIT, UNIT), UNIT)] = g
            sq[...] += fold(g.astype(jnp.float32))
            return
        away, here = halves(k, stage)
        outs[stage - 1][u] = total(away).astype(jnp.bfloat16)
        hop(u, k, stage).start()
        kept[stage - 1][u % 4] = total(here)

    def add_down(k, stage):
        down_hop(k, stage - 1).wait_recv()
        cols = pl.ds(*widths(dn.shape[1], 0)[k])

        def total(where):
            mine, other = (d_own, d_got) if stage == 1 else (d_kept[stage - 2], d_ins[stage - 2])
            at_ = (*where, everything, cols)
            return mine[at_].astype(jnp.float32) + other[at_].astype(jnp.float32)

        if stage == 4:
            g = total(()).astype(jnp.bfloat16)
            dn[:, cols] = g
            sq[...] += fold(g.astype(jnp.float32))
            return
        away, here = halves(k, stage)
        rest = (everything,) * (4 - stage)
        d_outs[stage - 1][(*rest, cols)] = total(away).astype(jnp.bfloat16)
        down_hop(k, stage).start()
        d_kept[stage - 1][(*rest, cols)] = total(here)

    def chunk(j):
        return pl.ds(pl.multiple_of(j * UNIT, UNIT), UNIT)

    def part_loads(j, p):
        rows = pl.ds(pl.multiple_of(p * part, part), part)
        pairs = ((gate, gates), (up, ups))
        return [pltpu.make_async_copy(s.at[rows, chunk(j)], t.at[p], p_sem.at[i, p]) for i, (s, t) in enumerate(pairs)]

    def weight_loads(j):
        slot = j % 2
        copies = [pltpu.make_async_copy(w_down.at[l, chunk(j)], wd.at[slot], w_sem.at[0, slot])]
        if with_da:
            for i, w in enumerate((w_gate, w_up)):
                copies.append(pltpu.make_async_copy(w.at[l, :, chunk(j)], wgu.at[slot, i], w_sem.at[1 + i, slot]))
        return copies

    def start(copies):
        for copy in copies:
            copy.start()

    def back_through(j):
        for copy in weight_loads(j):
            copy.wait()

        @pl.when(j + 1 < per)
        def _():
            start(weight_loads(j + 1))

        slot = j % 2

        def one(p, _):
            for copy in part_loads(j, p):
                copy.wait()
            rows = pl.ds(pl.multiple_of(p * part, part), part)
            dz = lax.dot_general(d[rows], wd[slot], (((1,), (1,)), ((), ())), preferred_element_type=jnp.float32)
            dz = dz.astype(jnp.bfloat16).astype(jnp.float32)
            g, u = gates[p], ups[p]
            sig = jax.nn.sigmoid(g)
            d_u = (dz * (g * sig)).astype(jnp.bfloat16)
            d_g = (dz * u * (sig * (1 + g * (1 - sig)))).astype(jnp.bfloat16)
            d_gu[0, rows] = d_g
            d_gu[1, rows] = d_u
            if with_da:
                da[rows] += lax.dot_general(
                    d_g, wgu[slot, 0], (((1,), (1,)), ((), ())), preferred_element_type=jnp.float32
                ) + lax.dot_general(d_u, wgu[slot, 1], (((1,), (1,)), ((), ())), preferred_element_type=jnp.float32)

            @pl.when(j + 1 < per)
            def _():
                start(part_loads(j + 1, p))

        lax.fori_loop(0, parts, one, None)

    def h_load(p):
        rows = pl.ds(pl.multiple_of(p * part, part), part)
        return pltpu.make_async_copy(h.at[rows], h_part.at[p % 2], h_sem.at[0, p % 2])

    def d_store(p):
        rows = pl.ds(pl.multiple_of(p * part, part), part)
        return pltpu.make_async_copy(h_part.at[p % 2], new_d.at[rows], h_sem.at[1, p % 2])

    def norm_back(p):
        h_load(p).wait()
        rows = pl.ds(pl.multiple_of(p * part, part), part)
        wide = h_part[p % 2].astype(jnp.float32)
        scale = lax.rsqrt(jnp.mean(wide * wide, -1, keepdims=True) + 1e-6)
        grad = da[rows]
        back = grad * scale - wide * (scale * scale * scale * jnp.mean(grad * wide, -1, keepdims=True))
        total = d[rows].astype(jnp.float32) + back.astype(jnp.bfloat16).astype(jnp.float32)
        h_part[p % 2] = total.astype(jnp.bfloat16)
        d_store(p).start()

        @pl.when(p + 2 < parts)
        def _():
            d_store(p).wait()
            h_load(p + 2).start()

    own = pltpu.make_async_copy(down.at[:, :, :, core], d_own, own_sem)
    own.start()
    start(weight_loads(0))
    for p in range(parts):
        start(part_loads(0, p))
    barrier = pltpu.get_barrier_semaphore()
    for stride in (1, *LINKS):
        pl.semaphore_signal(barrier, inc=1, device_id={"dp": flipped(me, stride)}, device_id_type=MESH)
    pl.semaphore_wait(barrier, 4)
    for k in range(3):
        down_hop(k, 0).start()
    sq[...] = jnp.zeros_like(sq)
    if with_da:
        da[...] = jnp.zeros_like(da)
    own.wait()

    def step(t, _):
        for stage, lag in reversed(list(enumerate(LAGS, 1))):
            u = t - lag
            for k in range(3):

                @pl.when((u >= 0) & (u < n_units) & ((u + 33) % 3 == k))
                def _():
                    add_up(u, k, stage)

        for stage, when in enumerate(DOWN_STEPS, 1):

            @pl.when(t == when)
            def _():
                for k in range(3):
                    add_down(k, stage)

        @pl.when(t < n_units)
        def _():
            @pl.when(t % 2 == 0)
            def _():
                back_through(t // 2)

            g = jnp.dot(a_t[...], d_gu[t % 2], preferred_element_type=jnp.float32).astype(jnp.bfloat16)
            tile[t % 3] = g.reshape(tile.shape[1:])
            hop(t, 0, 0).start()

        if with_da:

            @pl.when(t == n_units - 1)
            def _():
                for p in range(2):
                    h_load(p).start()

            @pl.when((t >= n_units) & (t < n_units + parts))
            def _():
                norm_back(t - n_units)

    lax.fori_loop(0, n_units + LAGS[-1], step, None)

    def drain(u, _):
        for stage in (1, 2, 3):
            hop(u, 0, stage).wait_send()

    lax.fori_loop(0, n_units, drain, None)
    for k in range(3):
        for stage in range(4):
            down_hop(k, stage).wait_send()
    if with_da:
        for p in (parts - 2, parts - 1):
            d_store(p).wait()


def reduce_layer(a_t, d, down, gate, up, w_down, l, h, weights, collective_id):
    width, tokens = a_t.shape
    ff = gate.shape[1]
    per, rows, d_rows, with_da = ff // UNIT, width // 16, ff // 16, weights is not None
    n_units, part = 2 * per, tokens // 4
    vmem, hbm = pl.BlockSpec(memory_space=pltpu.VMEM), pl.BlockSpec(memory_space=pl.ANY)
    dma, b16, f32 = pltpu.SemaphoreType.DMA, jnp.bfloat16, jnp.float32
    return pl.pallas_call(
        functools.partial(reduce_kernel, per, l, with_da),
        out_shape=[
            jax.ShapeDtypeStruct((rows, 2 * ff), b16),
            jax.ShapeDtypeStruct((d_rows, width), b16),
            jax.ShapeDtypeStruct((8, 128), f32),
        ]
        + [jax.ShapeDtypeStruct((tokens, width), b16)] * with_da,
        in_specs=[vmem] * 2 + [hbm] * (7 if with_da else 4),
        out_specs=[vmem] * 3 + [hbm] * with_da,
        scratch_shapes=[
            pltpu.VMEM((3, 2, 2, 2, 2, rows, UNIT), b16),
            pltpu.VMEM((4, 2, 2, 2, rows, UNIT), b16),
            pltpu.VMEM((4, 2, 2, rows, UNIT), f32),
            pltpu.VMEM((4, 2, rows, UNIT), f32),
            pltpu.VMEM((4, rows, UNIT), f32),
        ]
        + [pltpu.VMEM((slots, *lead, rows, UNIT), b16) for slots in (n_units, 6) for lead in ((2, 2), (2,), ())]
        + [pltpu.VMEM((2, 2, 2, d_rows, width), b16)] * 2
        + [pltpu.VMEM((2, 2, d_rows, width), f32), pltpu.VMEM((2, d_rows, width), f32), pltpu.VMEM((d_rows, width), f32)]
        + [pltpu.VMEM((2, 2, d_rows, width), b16), pltpu.VMEM((2, d_rows, width), b16), pltpu.VMEM((d_rows, width), b16)] * 2
        + [pltpu.VMEM((4, part, UNIT), f32)] * 2
        + [
            pltpu.VMEM((2, tokens, UNIT), b16),
            pltpu.VMEM((2, UNIT, width), b16),
            dma((2, 4)),
            dma((3, 2)),
            dma((4, n_units)),
            dma((4, n_units)),
            dma((4, 3)),
            dma((4, 3)),
            dma(()),
        ]
        + [
            pltpu.VMEM((tokens, width), f32),
            pltpu.VMEM((2, 2, width, UNIT), b16),
            pltpu.VMEM((2, part, width), b16),
            dma((2, 2)),
        ]
        * with_da,
        compiler_params=pltpu.CompilerParams(collective_id=collective_id, has_side_effects=True, vmem_limit_bytes=63 * 2**20),
        name=f"reduce_layer_{collective_id}",
    )(a_t, d, down.reshape(2, 2, 2, 2, d_rows, width), gate, up, w_down, *((*weights, h) if with_da else ()))


def solution(mesh):
    n = mesh.shape["dp"]

    def step(x, dy, w_gate, w_up, w_down, *moments):
        m, v = moments[:3], moments[3:]
        layers = w_gate.shape[0]
        h = x[0]
        saved = []
        for l in range(layers):
            last = l + 1 == layers
            gate, up, z_t, a_t, *new_h = forward_layer(h, w_gate, w_up, w_down, l, last)
            saved.append((h, a_t, gate, up, z_t))
            h = h if last else new_h[0]
        d = dy[0]
        summed, squares = [None] * layers, 0.0
        for l in reversed(range(layers)):
            h, a_t, gate, up, z_t = saved[l]
            down = dot(z_t, d, ((1,), (0,))).astype(jnp.bfloat16)
            weights = (w_gate, w_up) if l else None
            gu, dn, sq, *new_d = reduce_layer(a_t, d, down, gate, up, w_down, l, h, weights, l + 1)
            summed[l] = (gu, dn)
            squares = squares + sq
            if l:
                d = new_d[0]

        gu, dn = zip(*summed, strict=True)
        count = sum(t.size for t in m) * n
        return tuple(step_and_gather(squares, gu, dn, (w_gate, w_up, w_down), m, v, count))

    seq, whole, rows = P(("rep", "dp"), None, None), P(), P(None, "dp", None)
    return jax.shard_map(
        step,
        mesh=mesh,
        in_specs=(seq, seq) + (whole,) * 3 + (rows,) * 6,
        out_specs=(P("rep", None, None),) * 3 + (P("rep", "dp", None),) * 6,
        check_vma=False,
    )
```

```python
import functools

import jax
import jax.numpy as jnp
from jax import lax
from jax.experimental import pallas as pl
from jax.experimental.pallas import tpu as pltpu
from jax.sharding import PartitionSpec as P

MESH = pl.DeviceIdType.MESH

NAMES = ("w_gate", "w_up", "w_down")


def dot(a, b, dims):
    return lax.dot_general(a, b, (dims, ((), ())), preferred_element_type=jnp.float32)


LINKS = (8, 4, 2)


def flipped(me, stride):
    return me + stride - 2 * stride * ((me // stride) % 2)


def widths(columns, turn):
    lanes = columns // 128
    sizes = [128 * ((lanes + (k + turn) % 3) // 3) for k in range(3)]
    starts = [0, sizes[0], sizes[0] + sizes[1]]
    return list(zip(starts, sizes))


def gather_kernel(shapes, count, sq, *refs):
    n_mat, layers, ff = len(shapes), shapes[0][0], shapes[0][2]
    gu, dn, refs = refs[:layers], refs[layers : 2 * layers], refs[2 * layers :]
    w, m, v, new_w, new_m, new_v, own_w, out_w, out_m, out_v = (refs[i * n_mat : (i + 1) * n_mat] for i in range(10))
    squares, sq_send, sq_recv, in_sem, keep_sem, mv_sem, ici_send, ici_recv, d2d_send, d2d_recv = refs[10 * n_mat :]
    me = lax.axis_index("dp")
    at = [(me // s) % 2 for s in LINKS]
    core = me % 2
    units = [(i, l) for l in reversed(range(shapes[0][0])) for i in range(n_mat)]

    loads = [
        [
            pltpu.make_async_copy(w[i].at[l, me], own_w[i].at[l], in_sem.at[u, 0]),
            pltpu.make_async_copy(m[i].at[l], out_m[i].at[l], in_sem.at[u, 1]),
            pltpu.make_async_copy(v[i].at[l], out_v[i].at[l], in_sem.at[u, 2]),
        ]
        for u, (i, l) in enumerate(units)
    ]
    for copies in loads:
        for copy in copies:
            copy.start()
    barrier = pltpu.get_barrier_semaphore()
    for k in range(1, 16):
        pl.semaphore_signal(barrier, inc=1, device_id={"dp": (me + k) % 16}, device_id_type=MESH)
    pl.semaphore_wait(barrier, 15)

    sends = []
    for k in range(1, 16):
        copy = pltpu.make_async_remote_copy(
            sq, squares.at[me], sq_send.at[k], sq_recv.at[k], device_id={"dp": (me + k) % 16}, device_id_type=MESH
        )
        copy.start()
        sends.append(copy)
    squares[me] = sq[...]
    for copy in sends:
        copy.wait_recv()
    total = jnp.sum(jnp.sum(squares[...], axis=0), axis=(0, 1), keepdims=True)
    factor = jnp.minimum(1.0, 0.5 * lax.rsqrt(total / count + 1e-30))

    def ici(u, k, phase, i, l, cols):
        p, q, r = k, (k + 1) % 3, (k + 2) % 3
        where = list(at)
        for d in (p, q)[:phase]:
            where[d] = pl.ds(0, 2)
        there = new_w[i].at[l, where[0], where[1], where[2], core, :, pl.ds(*cols)]
        here = out_w[i].at[l, :, pl.ds(*cols)] if phase == 0 else there
        return pltpu.make_async_remote_copy(
            here,
            there,
            ici_send.at[3 * u + k, phase],
            ici_recv.at[3 * u + k, phase],
            device_id={"dp": flipped(me, LINKS[(p, q, r)[phase]])},
            device_id_type=MESH,
        )

    def d2d(u, k, piece, i, l, cols):
        order = (k, (k + 1) % 3, (k + 2) % 3)
        where = list(at)
        for d in order[: max(piece - 1, 0)]:
            where[d] = pl.ds(0, 2)
        if piece:
            where[order[piece - 1]] = 1 - at[order[piece - 1]]
        there = new_w[i].at[l, where[0], where[1], where[2], core, :, pl.ds(*cols)]
        here = out_w[i].at[l, :, pl.ds(*cols)] if piece == 0 else there
        return pltpu.make_async_remote_copy(
            here,
            there,
            d2d_send.at[3 * u + k, piece],
            d2d_recv.at[3 * u + k, piece],
            device_id={"dp": flipped(me, 1)},
            device_id_type=MESH,
        )

    moved, kept, stores = [], [], []
    for u, (i, l) in enumerate(units):
        for copy in loads[u]:
            copy.wait()
        g = dn[l][...] if i == 2 else gu[l][:, i * ff : (i + 1) * ff]
        clipped = g.astype(jnp.float32) * factor
        mm = 0.9 * out_m[i][l] + 0.1 * clipped
        vv = 0.95 * out_v[i][l] + 0.05 * clipped * clipped
        old = own_w[i][l].astype(jnp.float32)
        out_w[i][l] = (old - 0.02 * (mm * lax.rsqrt(vv + 1e-8) + 0.1 * old)).astype(jnp.bfloat16)
        out_m[i][l] = mm
        out_v[i][l] = vv
        for k, cols in enumerate(widths(shapes[i][2], u)):
            for copy in (ici(u, k, 0, i, l, cols), d2d(u, k, 0, i, l, cols)):
                copy.start()
                moved.append(copy)
        keep = pltpu.make_async_copy(out_w[i].at[l], new_w[i].at[l, at[0], at[1], at[2], core], keep_sem.at[u])
        keep.start()
        kept.append(keep)
        for j, (out, new) in enumerate(((out_m, new_m), (out_v, new_v))):
            store = pltpu.make_async_copy(out[i].at[l], new[i].at[l], mv_sem.at[u, j])
            store.start()
            stores.append(store)
    for keep in kept:
        keep.wait()
    for phase in range(3):
        for u, (i, l) in enumerate(units):
            for k, cols in enumerate(widths(shapes[i][2], u)):
                ici(u, k, phase, i, l, cols).wait_recv()
                follow = [d2d(u, k, phase + 1, i, l, cols)]
                if phase < 2:
                    follow.insert(0, ici(u, k, phase + 1, i, l, cols))
                for copy in follow:
                    copy.start()
                    moved.append(copy)
    for u, (i, l) in enumerate(units):
        for k, cols in enumerate(widths(shapes[i][2], u)):
            for piece in range(4):
                d2d(u, k, piece, i, l, cols).wait_recv()
    for copy in moved + sends:
        copy.wait_send()
    for store in stores:
        store.wait()


def step_and_gather(sq, gu, dn, w, m, v, count):
    shapes = [t.shape for t in m]
    n_units = sum(s[0] for s in shapes)
    blocks = [t.reshape(t.shape[0], 16, -1, t.shape[2]) for t in w]
    vmem, hbm = pl.BlockSpec(memory_space=pltpu.VMEM), pl.BlockSpec(memory_space=pl.ANY)
    dma = pltpu.SemaphoreType.DMA
    out = pl.pallas_call(
        functools.partial(gather_kernel, shapes, count),
        out_shape=[jax.ShapeDtypeStruct((s[0], 2, 2, 2, 2) + s[1:], jnp.bfloat16) for s in shapes]
        + [jax.ShapeDtypeStruct(s, jnp.float32) for s in shapes] * 2,
        in_specs=[vmem] * (1 + len(gu) + len(dn)) + [hbm] * 9,
        out_specs=[hbm] * 9,
        scratch_shapes=[pltpu.VMEM(s, jnp.bfloat16) for s in shapes] * 2
        + [pltpu.VMEM(s, jnp.float32) for s in shapes] * 2
        + [
            pltpu.VMEM((16, 8, 128), jnp.float32),
            dma((16,)),
            dma((16,)),
            dma((n_units, 3)),
            dma((n_units,)),
            dma((n_units, 2)),
            dma((3 * n_units, 3)),
            dma((3 * n_units, 3)),
            dma((3 * n_units, 4)),
            dma((3 * n_units, 4)),
        ],
        compiler_params=pltpu.CompilerParams(collective_id=0, has_side_effects=True, vmem_limit_bytes=60 * 2**20),
        name="step_and_gather",
    )(sq, *gu, *dn, *blocks, *m, *v)
    return [t.reshape(old.shape) for t, old in zip(out[:3], w)] + list(out[3:])


PARTS = 2
UNIT = 256
LAGS = (2, 7, 12, 17)
DOWN_STEPS = (3, 11, 17, 22)


def forward_kernel(last, h, w_gate, w_up, *refs):
    if last:
        gate, up, z_t, a_t, a = refs
    else:
        w_down, gate, up, z_t, a_t, new_h, a, total = refs
    j, part = pl.program_id(0), h.shape[0] // PARTS

    def over_parts(body):
        lax.fori_loop(0, PARTS, lambda p, _: body(pl.ds(pl.multiple_of(p * part, part), part)), None)

    @pl.when(j == 0)
    def _():
        def norm(rows):
            wide = h[rows].astype(jnp.float32)
            scale = lax.rsqrt(jnp.mean(wide * wide, -1, keepdims=True) + 1e-6)
            a[rows] = (wide * scale).astype(jnp.bfloat16)
            a_t[:, rows] = a[rows].T
            if not last:
                total[rows] = jnp.zeros((part, total.shape[1]), jnp.float32)

        over_parts(norm)

    def hidden(rows):
        g = jnp.dot(a[rows], w_gate[...], preferred_element_type=jnp.float32)
        u = jnp.dot(a[rows], w_up[...], preferred_element_type=jnp.float32)
        gate[rows] = g
        up[rows] = u
        z = (g * logistic(g) * u).astype(jnp.bfloat16)
        z_t[:, rows] = z.T
        if not last:
            total[rows] += jnp.dot(z, w_down[...], preferred_element_type=jnp.float32)

    over_parts(hidden)
    if not last:

        @pl.when(j == pl.num_programs(0) - 1)
        def _():
            def leave(rows):
                new_h[rows] = (h[rows].astype(jnp.float32) + total[rows].astype(jnp.bfloat16).astype(jnp.float32)).astype(jnp.bfloat16)

            over_parts(leave)


def forward_layer(h, w_gate, w_up, w_down, l, last):
    tokens, d = h.shape
    ff = w_gate.shape[2]
    b16, f32 = jnp.bfloat16, jnp.float32
    whole = lambda shape: pl.BlockSpec(shape, lambda j: (0, 0))
    column = pl.BlockSpec((None, d, UNIT), lambda j: (l, 0, j))
    hidden = pl.BlockSpec((tokens, UNIT), lambda j: (0, j))
    return pl.pallas_call(
        functools.partial(forward_kernel, last),
        grid=(ff // UNIT,),
        out_shape=[jax.ShapeDtypeStruct((tokens, ff), f32)] * 2
        + [jax.ShapeDtypeStruct((ff, tokens), b16), jax.ShapeDtypeStruct((d, tokens), b16)]
        + [jax.ShapeDtypeStruct((tokens, d), b16)] * (not last),
        in_specs=[whole((tokens, d)), column, column]
        + [pl.BlockSpec((None, UNIT, d), lambda j: (l, j, 0))] * (not last),
        out_specs=[hidden, hidden, pl.BlockSpec((UNIT, tokens), lambda j: (j, 0)), whole((d, tokens))]
        + [whole((tokens, d))] * (not last),
        scratch_shapes=[pltpu.VMEM((tokens, d), b16)] + [pltpu.VMEM((tokens, d), f32)] * (not last),
        compiler_params=pltpu.CompilerParams(dimension_semantics=("arbitrary",), vmem_limit_bytes=60 * 2**20),
        name=f"forward_layer_{l}",
    )(h, w_gate, w_up, *(() if last else (w_down,)))


def logistic(g):
    return 0.5 * jnp.tanh(0.5 * g) + 0.5


def fold(t):
    t = jnp.sum(jnp.square(t).reshape(-1, 8, t.shape[-1]), axis=0)
    return sum(t[:, j : j + 128] for j in range(0, t.shape[-1], 128))


def reduce_kernel(per, l, with_da, *refs):
    a_t_hbm, d_hbm, down, gate, up, w_down, *refs = refs
    if with_da:
        w_gate, w_up, h, *refs = refs
    gu, dn, sq, *refs = refs
    if with_da:
        new_d, *refs = refs
    tile, got, kept1, kept2, kept3, out1, out2, out3, in1, in2, in3 = refs[:11]
    d_own, d_got, d_kept1, d_kept2, d_kept3, d_out1, d_out2, d_out3, d_in1, d_in2, d_in3 = refs[11:22]
    a_t, d, gates, ups, d_gu, wd, p_sem, w_sem, send, recv, d_send, d_recv, own_sem, whole_sem, *refs = refs[22:]
    if with_da:
        da, wgu, h_part, h_sem = refs
    kept, outs, ins = (kept1, kept2, kept3), (out1, out2, out3), (in1, in2, in3)
    d_kept, d_outs, d_ins = (d_kept1, d_kept2, d_kept3), (d_out1, d_out2, d_out3), (d_in1, d_in2, d_in3)
    n_units = 2 * per
    me = lax.axis_index("dp")
    at = [(me // s) % 2 for s in LINKS]
    core = me % 2
    everything = slice(None)
    part = gates.shape[1]
    parts = d.shape[0] // part

    def remote(src, dst, s, r, stride):
        return pltpu.make_async_remote_copy(src, dst, s, r, device_id={"dp": flipped(me, stride)}, device_id_type=MESH)

    def hop(u, k, stage):
        if stage == 0:
            return remote(tile.at[u % 3, :, :, :, 1 - core], got.at[u % 4], send.at[0, u], recv.at[0, u], 1)
        return remote(outs[stage - 1].at[u % 6], ins[stage - 1].at[u % 12], send.at[stage, u], recv.at[stage, u], LINKS[(k + stage - 1) % 3])

    def down_hop(k, stage):
        cols = pl.ds(*widths(dn.shape[1], 0)[k])
        if stage == 0:
            src, dst, stride = down.at[:, :, :, 1 - core, :, cols], d_got.at[:, :, :, :, cols], 1
        else:
            lead = (everything,) * (4 - stage)
            src, dst = d_outs[stage - 1].at[(*lead, cols)], d_ins[stage - 1].at[(*lead, cols)]
            stride = LINKS[(k + stage - 1) % 3]
        return remote(src, dst, d_send.at[stage, k], d_recv.at[stage, k], stride)

    def halves(k, stage):
        axes = [d for d in range(3) if d not in [(k + j) % 3 for j in range(stage - 1)]]
        d = (k + stage - 1) % 3
        return [tuple(side if axis == d else everything for axis in axes) for side in (1 - at[d], at[d])]

    def add_up(u, k, stage):
        hop(u, k, stage - 1).wait_recv()
        if stage == 1:
            hop(u, k, 0).wait_send()

        def total(where):
            if stage == 1:
                mine, other = tile[(u % 3, *where, core)], got[(u % 4, *where)]
            else:
                mine, other = kept[stage - 2][(u % 6, *where)], ins[stage - 2][(u % 12, *where)]
            return mine.astype(jnp.float32) + other.astype(jnp.float32)

        if stage == 4:
            g = total(()).astype(jnp.bfloat16)
            gu[:, pl.ds(pl.multiple_of((u % 2) * per * UNIT + (u // 2) * UNIT, UNIT), UNIT)] = g
            sq[...] += fold(g.astype(jnp.float32))
            return
        away, here = halves(k, stage)

        @pl.when(u >= 6)
        def _():
            hop(u - 6, k, stage).wait_send()

        outs[stage - 1][u % 6] = total(away).astype(jnp.bfloat16)
        hop(u, k, stage).start()
        kept[stage - 1][u % 6] = total(here)

    def add_down(k, stage):
        down_hop(k, stage - 1).wait_recv()
        cols = pl.ds(*widths(dn.shape[1], 0)[k])

        def total(where):
            mine, other = (d_own, d_got) if stage == 1 else (d_kept[stage - 2], d_ins[stage - 2])
            at_ = (*where, everything, cols)
            return mine[at_].astype(jnp.float32) + other[at_].astype(jnp.float32)

        if stage == 4:
            g = total(()).astype(jnp.bfloat16)
            dn[:, cols] = g
            sq[...] += fold(g.astype(jnp.float32))
            return
        away, here = halves(k, stage)
        rest = (everything,) * (4 - stage)
        d_outs[stage - 1][(*rest, cols)] = total(away).astype(jnp.bfloat16)
        down_hop(k, stage).start()
        d_kept[stage - 1][(*rest, cols)] = total(here)

    def chunk(j):
        return pl.ds(pl.multiple_of(j * UNIT, UNIT), UNIT)

    def part_loads(j, p):
        rows = pl.ds(pl.multiple_of(p * part, part), part)
        pairs = ((gate, gates), (up, ups))
        return [pltpu.make_async_copy(s.at[rows, chunk(j)], t.at[p], p_sem.at[i, p]) for i, (s, t) in enumerate(pairs)]

    def weight_loads(j):
        slot = j % 2
        copies = [pltpu.make_async_copy(w_down.at[l, chunk(j)], wd.at[slot], w_sem.at[0, slot])]
        if with_da:
            for i, w in enumerate((w_gate, w_up)):
                copies.append(pltpu.make_async_copy(w.at[l, :, chunk(j)], wgu.at[slot, i], w_sem.at[1 + i, slot]))
        return copies

    def start(copies):
        for copy in copies:
            copy.start()

    def back_through(j):
        for copy in weight_loads(j):
            copy.wait()

        @pl.when(j + 1 < per)
        def _():
            start(weight_loads(j + 1))

        slot = j % 2

        def one(p, _):
            for copy in part_loads(j, p):
                copy.wait()
            rows = pl.ds(pl.multiple_of(p * part, part), part)
            dz = lax.dot_general(d[rows], wd[slot], (((1,), (1,)), ((), ())), preferred_element_type=jnp.float32)
            dz = dz.astype(jnp.bfloat16).astype(jnp.float32)
            g, u = gates[p], ups[p]
            sig = logistic(g)
            silu = g * sig
            d_u = (dz * silu).astype(jnp.bfloat16)
            d_g = (dz * u * (sig + silu * (1 - sig))).astype(jnp.bfloat16)
            d_gu[0, rows] = d_g
            d_gu[1, rows] = d_u
            if with_da:
                da[rows] += lax.dot_general(
                    d_g, wgu[slot, 0], (((1,), (1,)), ((), ())), preferred_element_type=jnp.float32
                ) + lax.dot_general(d_u, wgu[slot, 1], (((1,), (1,)), ((), ())), preferred_element_type=jnp.float32)

            @pl.when(j + 1 < per)
            def _():
                start(part_loads(j + 1, p))

        lax.fori_loop(0, parts, one, None)

    if with_da:
        block = h_part.shape[1]
        blocks = d.shape[0] // block

    def h_load(p):
        rows = pl.ds(pl.multiple_of(p * block, block), block)
        return pltpu.make_async_copy(h.at[rows], h_part.at[p % 2], h_sem.at[0, p % 2])

    def d_store(p):
        rows = pl.ds(pl.multiple_of(p * block, block), block)
        return pltpu.make_async_copy(h_part.at[p % 2], new_d.at[rows], h_sem.at[1, p % 2])

    def norm_back(p):
        h_load(p).wait()
        rows = pl.ds(pl.multiple_of(p * block, block), block)
        wide = h_part[p % 2].astype(jnp.float32)
        scale = lax.rsqrt(jnp.mean(wide * wide, -1, keepdims=True) + 1e-6)
        grad = da[rows]
        back = grad * scale - wide * (scale * scale * scale * jnp.mean(grad * wide, -1, keepdims=True))
        total = d[rows].astype(jnp.float32) + back.astype(jnp.bfloat16).astype(jnp.float32)
        h_part[p % 2] = total.astype(jnp.bfloat16)
        d_store(p).start()

        @pl.when(p + 2 < blocks)
        def _():
            d_store(p).wait()
            h_load(p + 2).start()

    own = pltpu.make_async_copy(down.at[:, :, :, core], d_own, own_sem)
    wholes = [pltpu.make_async_copy(s, t, whole_sem.at[i]) for i, (s, t) in enumerate(((d_hbm, d), (a_t_hbm, a_t)))]
    wholes[0].start()
    start(weight_loads(0))
    for p in range(parts):
        start(part_loads(0, p))
    own.start()
    wholes[1].start()
    barrier = pltpu.get_barrier_semaphore()
    for stride in (1, *LINKS):
        pl.semaphore_signal(barrier, inc=1, device_id={"dp": flipped(me, stride)}, device_id_type=MESH)
    pl.semaphore_wait(barrier, 4)
    for k in range(3):
        down_hop(k, 0).start()
    sq[...] = jnp.zeros_like(sq)
    if with_da:
        da[...] = jnp.zeros_like(da)
    own.wait()
    for copy in wholes:
        copy.wait()

    def step(t, _):
        for stage, lag in reversed(list(enumerate(LAGS, 1))):
            u = t - lag
            for k in range(3):

                @pl.when((u >= 0) & (u < n_units) & ((u + 33) % 3 == k))
                def _():
                    add_up(u, k, stage)

        for stage, when in enumerate(DOWN_STEPS, 1):

            @pl.when(t == when)
            def _():
                for k in range(3):
                    add_down(k, stage)

        @pl.when(t < n_units)
        def _():
            @pl.when(t % 2 == 0)
            def _():
                back_through(t // 2)

            g = jnp.dot(a_t[...], d_gu[t % 2], preferred_element_type=jnp.float32).astype(jnp.bfloat16)
            tile[t % 3] = g.reshape(tile.shape[1:])
            hop(t, 0, 0).start()

        if with_da:

            @pl.when(t == n_units - 1)
            def _():
                for p in range(2):
                    h_load(p).start()

            @pl.when((t >= n_units) & (t < n_units + blocks))
            def _():
                norm_back(t - n_units)

    lax.fori_loop(0, n_units + LAGS[-1], step, None)

    def drain(u, _):
        for stage in (1, 2, 3):
            hop(u, 0, stage).wait_send()

    lax.fori_loop(n_units - 6, n_units, drain, None)
    for k in range(3):
        for stage in range(4):
            down_hop(k, stage).wait_send()
    if with_da:
        for p in (blocks - 2, blocks - 1):
            d_store(p).wait()


def reduce_layer(a_t, d, down, gate, up, w_down, l, h, weights, collective_id):
    width, tokens = a_t.shape
    ff = gate.shape[1]
    per, rows, d_rows, with_da = ff // UNIT, width // 16, ff // 16, weights is not None
    n_units, part = 2 * per, tokens // PARTS
    vmem, hbm = pl.BlockSpec(memory_space=pltpu.VMEM), pl.BlockSpec(memory_space=pl.ANY)
    dma, b16, f32 = pltpu.SemaphoreType.DMA, jnp.bfloat16, jnp.float32
    return pl.pallas_call(
        functools.partial(reduce_kernel, per, l, with_da),
        out_shape=[
            jax.ShapeDtypeStruct((rows, 2 * ff), b16),
            jax.ShapeDtypeStruct((d_rows, width), b16),
            jax.ShapeDtypeStruct((8, 128), f32),
        ]
        + [jax.ShapeDtypeStruct((tokens, width), b16)] * with_da,
        in_specs=[hbm] * (9 if with_da else 6),
        out_specs=[vmem] * 3 + [hbm] * with_da,
        scratch_shapes=[
            pltpu.VMEM((3, 2, 2, 2, 2, rows, UNIT), b16),
            pltpu.VMEM((4, 2, 2, 2, rows, UNIT), b16),
            pltpu.VMEM((6, 2, 2, rows, UNIT), f32),
            pltpu.VMEM((6, 2, rows, UNIT), f32),
            pltpu.VMEM((6, rows, UNIT), f32),
        ]
        + [pltpu.VMEM((slots, *lead, rows, UNIT), b16) for slots in (6, 12) for lead in ((2, 2), (2,), ())]
        + [pltpu.VMEM((2, 2, 2, d_rows, width), b16)] * 2
        + [pltpu.VMEM((2, 2, d_rows, width), f32), pltpu.VMEM((2, d_rows, width), f32), pltpu.VMEM((d_rows, width), f32)]
        + [pltpu.VMEM((2, 2, d_rows, width), b16), pltpu.VMEM((2, d_rows, width), b16), pltpu.VMEM((d_rows, width), b16)] * 2
        + [pltpu.VMEM((width, tokens), b16), pltpu.VMEM((tokens, width), b16)]
        + [pltpu.VMEM((PARTS, part, UNIT), f32)] * 2
        + [
            pltpu.VMEM((2, tokens, UNIT), b16),
            pltpu.VMEM((2, UNIT, width), b16),
            dma((2, PARTS)),
            dma((3, 2)),
            dma((4, n_units)),
            dma((4, n_units)),
            dma((4, 3)),
            dma((4, 3)),
            dma(()),
            dma((2,)),
        ]
        + [
            pltpu.VMEM((tokens, width), f32),
            pltpu.VMEM((2, 2, width, UNIT), b16),
            pltpu.VMEM((2, tokens // 8, width), b16),
            dma((2, 2)),
        ]
        * with_da,
        compiler_params=pltpu.CompilerParams(collective_id=collective_id, has_side_effects=True, vmem_limit_bytes=63 * 2**20),
        name=f"reduce_layer_{collective_id}",
    )(a_t, d, down.reshape(2, 2, 2, 2, d_rows, width), gate, up, w_down, *((*weights, h) if with_da else ()))


def solution(mesh):
    n = mesh.shape["dp"]

    def step(x, dy, w_gate, w_up, w_down, *moments):
        m, v = moments[:3], moments[3:]
        layers = w_gate.shape[0]
        h = x[0]
        saved = []
        for l in range(layers):
            last = l + 1 == layers
            gate, up, z_t, a_t, *new_h = forward_layer(h, w_gate, w_up, w_down, l, last)
            saved.append((h, a_t, gate, up, z_t))
            h = h if last else new_h[0]
        d = dy[0]
        summed, squares = [None] * layers, 0.0
        for l in reversed(range(layers)):
            h, a_t, gate, up, z_t = saved[l]
            down = dot(z_t, d, ((1,), (0,))).astype(jnp.bfloat16)
            weights = (w_gate, w_up) if l else None
            gu, dn, sq, *new_d = reduce_layer(a_t, d, down, gate, up, w_down, l, h, weights, l + 1)
            summed[l] = (gu, dn)
            squares = squares + sq
            if l:
                d = new_d[0]

        gu, dn = zip(*summed, strict=True)
        count = sum(t.size for t in m) * n
        return tuple(step_and_gather(squares, gu, dn, (w_gate, w_up, w_down), m, v, count))

    seq, whole, rows = P(("rep", "dp"), None, None), P(), P(None, "dp", None)
    return jax.shard_map(
        step,
        mesh=mesh,
        in_specs=(seq, seq) + (whole,) * 3 + (rows,) * 6,
        out_specs=(P("rep", None, None),) * 3 + (P("rep", "dp", None),) * 6,
        check_vma=False,
    )
```
